32 devices in a mesh: groups: 2 (over y), seq: 4 (over z), rep: 4 (over x, core).
Axes of the slice: x: 2, y: 2, z: 4, core: 2. Of those that a mesh axis runs over, the one named last changes fastest.
Arguments:
- queries: bfloat16 [128, 2048], P(('groups', 'seq'), 'rep'), parts along dimension 0, may hold values from -128 to 128
- keys_new: bfloat16 [128, 512], P(('groups', 'seq'), 'rep'), parts along dimension 0, may hold values from -4 to 4
- values_new: bfloat16 [128, 512], P(('groups', 'seq'), 'rep'), parts along dimension 0, may hold values from -6 to 6
- keys_past: bfloat16 [2048, 512], P(('groups', 'seq'), 'rep'), parts along dimension 0, may hold values from -4 to 4
- values_past: bfloat16 [2048, 512], P(('groups', 'seq'), 'rep'), parts along dimension 0, may hold values from -6 to 6
- block_order: int32 [8], P('groups'), parts along dimension 0, may hold values from 0 to 3, each once
- residual: bfloat16 [128, 4096], P(('groups', 'seq'), 'rep'), parts along dimension 0, may hold values from -6 to 6
- out_proj: bfloat16 [2048, 4096], P('seq', 'rep'), may hold values from -0.125 to 0.125
- norm_gain: float32 [4096], replicated, may hold values from 0.5 to 1.5
- router: float32 [4096, 4], replicated, may hold values from -0.09375 to 0.09375
- w_gate: bfloat16 [4, 4096, 8192], P('rep', None, 'seq'), may hold values from -0.09375 to 0.09375
- w_up: bfloat16 [4, 4096, 8192], P('rep', None, 'seq'), may hold values from -0.09375 to 0.09375
- w_down: bfloat16 [4, 8192, 4096], P('rep', 'seq'), may hold values from -0.0625 to 0.0625
- expert_ids: int32 [128, 2], P(('groups', 'seq')), parts along dimension 0, may hold values from 0 to 3, all different within a row; in each aligned block of 16 rows (0 to 15, 16 to 31, ...) at most 12 rows name the same one
Outputs:
- attended: bfloat16 [128, 4096], P(('groups', 'seq'), 'rep'), parts along dimension 0
- layer_out: bfloat16 [128, 4096], P(('groups', 'seq'), 'rep'), parts along dimension 0
- keys_cache: bfloat16 [128, 512], P(('groups', 'seq')), parts along dimension 0
- values_cache: bfloat16 [128, 512], P(('groups', 'seq')), parts along dimension 0
The draws below stay inside these ranges and needn't reach their ends.
There are 2 independent parts, one for each index of `groups`. The reference program is written for one: setup_inputs(seed, part) draws one part's arguments, and reference() takes and returns one part's arrays. A program takes and returns all parts, laid end to end along the dimension named above; an argument that names none is the same for every part. Nothing has to cross between parts.
Inputs may be any that keep to these rules, and one draw needn't show every extreme that they name: `block_order`: each block index 0 to 4 - 1 appears once. `expert_ids`: each row names 2 different experts; in the rows of one device (aligned blocks of 16 rows) no expert is named by more than 12 rows, and in some block one expert is named by exactly 12.
All inputs are finite; a program needn't handle non-finite values.
Results may differ from the reference program's by a relative error of at most 0.011.
Values may be sent and summed in bfloat16 or wider, within the bound.
A program may use at most 128 MiB of HBM per device.

```python
import math
import jax
import jax.numpy as jnp
import numpy as np
from jax import lax

D = 4096
HD = 128
Q_PER = 4
KV_HEADS = 4
HEADS = 16
EXPERTS = 4
TOP = 2
FF = 8192
TOK_DEV = 16
CAP = 12
HALVES = 1
S_NEW = 64
CTX = 1024
N_SEQ = 4


def drawn_pair(key):
    base = jax.random.fold_in(key, 11)
    key_seed, query_seed = jax.random.split(base)
    past_keys = jnp.clip(jax.random.normal(key_seed, (CTX, KV_HEADS * HD), jnp.float32), -4.0, 4.0)
    query_rows = jnp.clip(jax.random.normal(query_seed, (S_NEW, KV_HEADS * Q_PER * HD), jnp.float32), -4.0, 4.0)
    return (past_keys, query_rows)


def draw_queries(key, part):
    past_keys, query_rows = drawn_pair(key)
    return query_rows.astype(jnp.bfloat16)


def draw_keys_past(key, part):
    past_keys, query_rows = drawn_pair(key)
    return past_keys.astype(jnp.bfloat16)


def block_levels(own_key, shape, cuts, least, high):
    def one(dim, shards_of):
        draws = jax.random.uniform(jax.random.fold_in(jax.random.fold_in(own_key, 6), dim), (shards_of,), jnp.float32, least / len(cuts), high / len(cuts))
        return jnp.repeat(jnp.exp(draws), shape[dim] // shards_of).reshape((-1,) + (1,) * (len(shape) - dim - 1))

    loudness = one(*cuts[0])
    for cut in cuts[1:]:
        loudness = loudness * one(*cut)
    return loudness


def routed_block(key, own, number, rows, count, top, bound, lean):
    sequence = jax.random.permutation(key, count)
    heavy_load, usual = portions_of(count, rows * top, bound, lean, True), portions_of(count, rows * top, bound, lean, False)
    places = jnp.arange(count)

    def named(tallies, turn):
        used = int((tallies > 0).sum())
        fixed = max(1, used // 4)
        passed = fixed + (places - fixed + turn * (used - fixed)) % max(1, count - fixed)
        return jnp.zeros((count,), jnp.int32).at[sequence[jnp.where(places < fixed, places, passed)]].set(jnp.asarray(tallies, jnp.int32))

    tallies = jnp.where(number % 4 == 0, named(heavy_load, number // 4), named(usual, number - number // 4 - 1))
    mixed = jax.random.permutation(jax.random.fold_in(own, 3), count)
    giver, taker = mixed[0:count // 2 * 2:2], mixed[1:count // 2 * 2:2]
    room = jnp.minimum(tallies[giver] - 1, bound - tallies[taker]) // 2
    room = jnp.where((giver == sequence[0]) | (taker == sequence[0]) | (tallies[taker] == 0), 0, jnp.maximum(room, 0))
    passed = jax.random.randint(jax.random.fold_in(own, 4), (count // 2,), 0, 1 << 20) % (room + 1)
    tallies = tallies.at[giver].add(-passed).at[taker].add(passed)
    labels = jnp.searchsorted(jnp.cumsum(tallies), jnp.arange(rows * top), side="right").astype(jnp.int32)
    table = labels.reshape(top, rows).T
    table = table[jax.random.permutation(jax.random.fold_in(own, 1), rows)]
    turn = jax.random.randint(jax.random.fold_in(own, 2), (rows, 1), 0, top)
    return jnp.take_along_axis(table, (jnp.arange(top)[None, :] + turn) % top, axis=1)


def portions_of(amount, total, most, skew, full):
    loads = [(1 << 20) // math.isqrt(grade ** skew) + 1 for grade in range(1, amount + 1)]
    largest = most if full else min(most, max(-(-total // amount), total * loads[0] // sum(loads)))
    least = 1 if total - largest >= amount - 1 else 0
    given, spare = [largest] + [least] * (amount - 1), total - largest - least * (amount - 1)
    while spare > 0:
        movable = [i for i in range(1, amount) if given[i] < largest] or [i for i in range(1, amount) if given[i] < most]
        mass, remaining = sum([loads[i] for i in movable]), spare
        for i in movable:
            addition = min(most - given[i], max(1, remaining * loads[i] // mass), spare)
            given[i] = given[i] + addition
            spare = spare - addition
    return np.array(given)


def noise(stream_key, shape, scale, reach, cuts=(), kind=jnp.bfloat16):
    level = block_levels(stream_key, shape, cuts, -0.22, 0.18) if cuts else 1.0
    values = jax.random.normal(stream_key, shape, jnp.float32) * scale * level
    return jnp.minimum(jnp.maximum(values, -reach), reach).astype(kind)


def setup_inputs(seed: int = 0, part: int = 0) -> dict:
    streams_of = jax.random.split(jax.random.key(seed), 15)
    part_keys = jax.random.split(jax.random.fold_in(streams_of[14], part), 15)
    queries = draw_queries(jax.random.fold_in(jax.random.fold_in(streams_of[14], part), 71), part)
    keys_new = noise(part_keys[1], (S_NEW, KV_HEADS * HD), 1.0, 4.0, ((0, 4), (1, 4)))
    values_new = noise(part_keys[2], (S_NEW, KV_HEADS * HD), 1.0, 6.0, ((0, 4), (1, 4)))
    keys_past = draw_keys_past(jax.random.fold_in(jax.random.fold_in(streams_of[14], part), 71), part)
    values_past = noise(part_keys[4], (CTX, KV_HEADS * HD), 1.0, 6.0, ((0, 4), (1, 4)))
    block_order = jax.random.permutation(part_keys[5], N_SEQ).astype(jnp.int32)
    residual = noise(part_keys[6], (S_NEW, D), 1.0, 6.0, ((0, 4), (1, 4)))
    out_proj = noise(streams_of[7], (HEADS * HD, D), (HEADS * HD) ** -0.5, 0.125, ((0, 4), (1, 4)))
    norm_gain = jnp.clip(1.0 + 0.1 * jax.random.normal(streams_of[8], (D,), jnp.float32), 0.5, 1.5)
    router = noise(streams_of[9], (D, EXPERTS), D ** -0.5, 0.09375, (), jnp.float32)
    w_gate = noise(streams_of[10], (EXPERTS * HALVES, D, FF // HALVES), D ** -0.5, 0.09375, ((0, 4), (2, 4)))
    w_up = noise(streams_of[11], (EXPERTS * HALVES, D, FF // HALVES), D ** -0.5, 0.09375, ((0, 4), (2, 4)))
    w_down = noise(streams_of[12], (EXPERTS * HALVES, FF // HALVES, D), FF ** -0.5, 0.0625, ((0, 4), (1, 4)))
    expert_ids_keys = jax.random.split(jax.random.fold_in(part_keys[13], 1), S_NEW // TOK_DEV)
    expert_ids_turns = jax.random.permutation(jax.random.fold_in(part_keys[13], 3), S_NEW // TOK_DEV)
    expert_ids = jax.vmap(lambda own, number: routed_block(jax.random.fold_in(part_keys[13], 2), own, number, TOK_DEV, EXPERTS, TOP, CAP, 2))(expert_ids_keys, expert_ids_turns).reshape((S_NEW, TOP))
    return {"queries": queries, "keys_new": keys_new, "values_new": values_new, "keys_past": keys_past, "values_past": values_past, "block_order": block_order, "residual": residual, "out_proj": out_proj, "norm_gain": norm_gain, "router": router, "w_gate": w_gate, "w_up": w_up, "w_down": w_down, "expert_ids": expert_ids}


def reference(queries, keys_new, values_new, keys_past, values_past, block_order, residual, out_proj, norm_gain, router, w_gate, w_up, w_down, expert_ids):
    token_index = jnp.arange(S_NEW, dtype=jnp.int32)
    position = block_order[token_index // TOK_DEV] * TOK_DEV + token_index % TOK_DEV
    new_visible = position[None, :] <= position[:, None]
    row_visible = jnp.concatenate([jnp.ones((S_NEW, CTX), dtype=bool), new_visible], axis=1)
    row_visible = jnp.repeat(row_visible, Q_PER, axis=0)
    query_heads = queries.reshape(S_NEW, KV_HEADS, Q_PER, HD).transpose(1, 0, 2, 3).reshape(KV_HEADS, S_NEW * Q_PER, HD)
    keys_all = jnp.concatenate([keys_past, keys_new], axis=0).reshape(CTX + S_NEW, KV_HEADS, HD).transpose(1, 0, 2)
    values_all = jnp.concatenate([values_past, values_new], axis=0).reshape(CTX + S_NEW, KV_HEADS, HD).transpose(1, 0, 2)

    def one_head(operands):
        query_block, key_block, value_block = operands
        scores = jnp.dot(query_block, key_block.T, preferred_element_type=jnp.float32) * (1.0 / math.sqrt(HD))
        highest = lax.optimization_barrier(jnp.max(jnp.where(row_visible, scores, -jnp.inf), axis=1, keepdims=True))
        weights = jnp.where(row_visible, jnp.exp(scores - highest), 0.0)
        numerator = jnp.dot(weights.astype(jnp.bfloat16), value_block, preferred_element_type=jnp.float32)
        return (numerator / lax.optimization_barrier(jnp.sum(weights, axis=1, keepdims=True))).astype(jnp.bfloat16)
    heads_out = lax.map(one_head, (query_heads, keys_all, values_all))
    attended_heads = heads_out.reshape(KV_HEADS, S_NEW, Q_PER * HD).transpose(1, 0, 2).reshape(S_NEW, KV_HEADS * Q_PER * HD)
    projected = jnp.dot(attended_heads, out_proj, preferred_element_type=jnp.float32)
    attended = (residual.astype(jnp.float32) + projected).astype(jnp.bfloat16)
    features = attended.astype(jnp.float32)
    mean_square = lax.optimization_barrier(jnp.mean(features * features, axis=1, keepdims=True))
    normed = (features * norm_gain[None, :] * lax.rsqrt(mean_square + 1e-05)).astype(jnp.bfloat16)
    logits = jnp.dot(normed.astype(jnp.float32), router, precision=lax.Precision.HIGHEST)
    expert_range = jnp.arange(EXPERTS, dtype=jnp.int32)
    first_pick = (expert_ids[:, 0:1] == expert_range[None, :]).astype(jnp.float32)
    second_pick = (expert_ids[:, 1:2] == expert_range[None, :]).astype(jnp.float32)
    share_first = jax.nn.sigmoid(lax.optimization_barrier(jnp.sum(first_pick * logits, axis=1)) - lax.optimization_barrier(jnp.sum(second_pick * logits, axis=1)))
    token_share = share_first[:, None] * first_pick + (1.0 - share_first)[:, None] * second_pick
    block_count = HALVES * N_SEQ
    block_width = FF // block_count
    mixture = jnp.zeros((S_NEW, D), jnp.float32)

    def add_block(running_sum, operands):
        act_piece, down_piece = operands
        partial_sum = jnp.dot(act_piece, down_piece, preferred_element_type=jnp.float32)
        rounded = lax.optimization_barrier(partial_sum.astype(jnp.bfloat16))
        return (running_sum + rounded.astype(jnp.float32), None)
    for expert in range(EXPERTS):
        gate_full = jnp.concatenate([w_gate[half_index * EXPERTS + expert] for half_index in range(HALVES)], axis=1)
        up_full = jnp.concatenate([w_up[half_index * EXPERTS + expert] for half_index in range(HALVES)], axis=1)
        down_full = jnp.concatenate([w_down[half_index * EXPERTS + expert] for half_index in range(HALVES)], axis=0)
        gate_part = jnp.dot(normed, gate_full, preferred_element_type=jnp.float32)
        up_part = jnp.dot(normed, up_full, preferred_element_type=jnp.float32)
        activation = (jax.nn.silu(gate_part) * up_part).astype(jnp.bfloat16)
        act_blocks = activation.reshape(S_NEW, block_count, block_width).transpose(1, 0, 2)
        down_blocks = down_full.reshape(block_count, block_width, D)
        expert_out, ignored = lax.scan(add_block, jnp.zeros((S_NEW, D), jnp.float32), (act_blocks, down_blocks))
        mixture = mixture + token_share[:, expert:expert + 1] * expert_out
    layer_out = (features + mixture).astype(jnp.bfloat16)
    return (attended, layer_out, keys_new, values_new)
```

```python
import functools
import math

import jax
import jax.numpy as jnp
from jax import lax
from jax.experimental import pallas as pl
from jax.experimental.pallas import tpu as pltpu
from jax.sharding import PartitionSpec as P

EXPERTS = 4
CAP = 12


def block_lookup(owners, block_order):
    width = block_order.shape[0]
    hits = owners[:, None] == jnp.arange(width, dtype=jnp.int32)[None, :]
    return jnp.sum(jnp.where(hits, block_order[None, :], 0), axis=1)


def plain_body(
    queries,
    keys_new,
    values_new,
    keys_past,
    values_past,
    block_order,
    residual,
    out_proj,
    norm_gain,
    router,
    w_gate,
    w_up,
    w_down,
    expert_ids,
):
    seq_index = lax.axis_index("seq")
    rep_index = lax.axis_index("rep")
    rep_count = lax.axis_size("rep")
    tok_count = queries.shape[0]
    head_dim = keys_new.shape[1]
    q_per = queries.shape[1] // head_dim
    past_len = keys_past.shape[0]
    key_span = past_len + tok_count
    row_total = tok_count * q_per
    my_block = block_lookup(jnp.full((1,), seq_index, jnp.int32), block_order)[0]
    scaling = 1.0 / math.sqrt(head_dim)
    query_rows = queries.reshape(row_total, head_dim)
    query_pos = my_block * tok_count + jnp.arange(row_total, dtype=jnp.int32) // q_per
    keys_local = jnp.concatenate([keys_past, keys_new], axis=0)
    values_local = jnp.concatenate([values_past, values_new], axis=0)
    running = jnp.full((row_total,), -1e30, jnp.float32)
    key_piece = lax.all_gather(keys_local, "seq", axis=0, tiled=True)
    value_piece = lax.all_gather(values_local, "seq", axis=0, tiled=True)
    row_count = key_piece.shape[0]
    key_index = jnp.arange(row_count, dtype=jnp.int32)
    key_owner = key_index // key_span
    offset = key_index % key_span
    key_pos = block_lookup(key_owner, block_order) * tok_count + offset - past_len
    visible = (offset < past_len)[None, :] | (key_pos[None, :] <= query_pos[:, None])
    scores = jnp.dot(query_rows, key_piece.T, preferred_element_type=jnp.float32) * scaling
    highest = jnp.maximum(running, jnp.max(jnp.where(visible, scores, -1e30), axis=1))
    weights = jnp.where(visible, jnp.exp(scores - highest[:, None]), 0.0)
    totals = jnp.sum(weights, axis=1)
    numerator = jnp.dot(
        weights.astype(jnp.bfloat16), value_piece, preferred_element_type=jnp.float32
    )
    running, totals, numerator = (highest, totals, numerator)
    attn_local = (
        (numerator / totals[:, None]).reshape(tok_count, q_per * head_dim).astype(jnp.bfloat16)
    )
    attn_full, keys_cache, values_cache = (
        lax.all_gather(attn_local, "rep", axis=1, tiled=True),
        lax.all_gather(keys_new, "rep", axis=1, tiled=True),
        lax.all_gather(values_new, "rep", axis=1, tiled=True),
    )
    head_rows = lax.all_to_all(attn_full, "seq", split_axis=1, concat_axis=0, tiled=True)
    projected = lax.psum_scatter(
        jnp.dot(head_rows, out_proj, preferred_element_type=jnp.float32).astype(jnp.bfloat16),
        "seq",
        scatter_dimension=0,
        tiled=True,
    ).astype(jnp.float32)
    attended = (residual.astype(jnp.float32) + projected).astype(jnp.bfloat16)
    full_rows = lax.all_gather(attended, "rep", axis=1, tiled=True)
    features = full_rows.astype(jnp.float32)
    mean_square = jnp.mean(features * features, axis=1, keepdims=True)
    normed = (features * norm_gain[None, :] * lax.rsqrt(mean_square + 1e-05)).astype(jnp.bfloat16)
    logits = jnp.dot(normed.astype(jnp.float32), router, precision=lax.Precision.HIGHEST)
    expert_range = jnp.arange(EXPERTS, dtype=jnp.int32)
    first_pick = (expert_ids[:, 0:1] == expert_range[None, :]).astype(jnp.float32)
    second_pick = (expert_ids[:, 1:2] == expert_range[None, :]).astype(jnp.float32)
    share_first = jax.nn.sigmoid(
        jnp.sum(first_pick * logits, axis=1) - jnp.sum(second_pick * logits, axis=1)
    )
    token_share = share_first[:, None] * first_pick + (1.0 - share_first)[:, None] * second_pick
    member = first_pick + second_pick
    ranking = jnp.cumsum(member, axis=0) - member
    slot_range = jnp.arange(CAP, dtype=jnp.float32)
    selection = member.T[:, None, :] * (ranking.T[:, None, :] == slot_range[None, :, None]).astype(
        jnp.float32
    )
    mine_mask = (expert_range == rep_index % EXPERTS).astype(jnp.float32)
    my_selection = jnp.einsum("e,ejt->jt", mine_mask, selection)
    slot_rows = jnp.dot(
        my_selection.astype(jnp.bfloat16), normed, preferred_element_type=jnp.float32
    ).astype(jnp.bfloat16)
    gate_local = w_gate[0]
    up_local = w_up[0]
    down_local = w_down[0]
    piece = lax.all_gather(slot_rows, "seq", axis=0, tiled=True)
    gate_part = jnp.dot(piece, gate_local, preferred_element_type=jnp.float32)
    up_part = jnp.dot(piece, up_local, preferred_element_type=jnp.float32)
    hidden_slots = (jax.nn.silu(gate_part) * up_part).astype(jnp.bfloat16)
    expert_part = lax.psum_scatter(
        jnp.dot(hidden_slots, down_local, preferred_element_type=jnp.float32).astype(jnp.bfloat16),
        "seq",
        scatter_dimension=0,
        tiled=True,
    ).astype(jnp.float32)
    returned = lax.all_to_all(
        expert_part.astype(jnp.bfloat16), "rep", split_axis=1, concat_axis=0, tiled=True
    ).astype(expert_part.dtype)
    source_expert = jnp.arange(rep_count, dtype=jnp.int32) % EXPERTS
    source_pick = (source_expert[:, None] == expert_range[None, :]).astype(jnp.float32)
    combine = jnp.einsum("re,ejt,te->trj", source_pick, selection, token_share).reshape(
        tok_count, rep_count * CAP
    )
    moe_slice = jnp.dot(combine, returned, precision=lax.Precision.HIGHEST)
    layer_out = (attended.astype(jnp.float32) + moe_slice).astype(jnp.bfloat16)
    return (attended, layer_out, keys_cache, values_cache)


MESH = pl.DeviceIdType.MESH
STAT_ROWS = 8
F32 = jnp.float32
BF16 = jnp.bfloat16


def fused_kernel(
    n_seq,
    n_rep,
    order_hbm,
    q_hbm,
    kn_hbm,
    vn_hbm,
    kp_hbm,
    vp_hbm,
    res_hbm,
    gain_hbm,
    router_hbm,
    ids_hbm,
    proj_hbm,
    gate_hbm,
    up_hbm,
    down_hbm,
    att_out,
    layer_out,
    kc_out,
    vc_out,
    order_ref,
    q_ref,
    kn_ref,
    vn_ref,
    kp_ref,
    vp_ref,
    res_ref,
    gain_ref,
    router_ref,
    ids_ref,
    in_sem,
    wproj,
    wgate,
    wup,
    wdown,
    qall,
    idall,
    kcache,
    vcache,
    num_send,
    stat_send,
    num_all,
    stat_all,
    part_send,
    part_all,
    xall,
    gained,
    gate_acc,
    up_acc,
    inverse_ref,
    hidden,
    ysend,
    yall,
    zsend,
    zall,
    w_sem,
    small_send,
    small_recv,
    num_ssem,
    num_rsem,
    hand_ssem,
    pass_ssem,
    pass_rsem,
    part_ssem,
    part_rsem,
    x_ssem,
    x_rsem,
    y_ssem,
    y_rsem,
    z_ssem,
    z_rsem,
):
    group = lax.axis_index("groups")
    seq = lax.axis_index("seq")
    rep = lax.axis_index("rep")
    tok, width = q_ref.shape
    hd = kn_ref.shape[1]
    q_per = width // hd
    toks = tok * n_seq
    feat = res_ref.shape[1]

    chips = n_rep // 2
    chip, core = rep // 2, lax.rem(rep, 2)
    partner = chip * 2 + 1 - core

    def same_core(step):
        return lax.rem(chip + step, chips) * 2 + core

    def other_core(step):
        return lax.rem(chip + step, chips) * 2 + 1 - core

    def dev(s, r):
        return {"groups": group, "seq": s, "rep": r}

    def other(index, step, size):
        return lax.rem(index + step, size)

    def remote(src, dst, ssem, rsem, s, r):
        return pltpu.make_async_remote_copy(
            src_ref=src,
            dst_ref=dst,
            send_sem=ssem,
            recv_sem=rsem,
            device_id=dev(s, r),
            device_id_type=MESH,
        )

    def rows_of(index):
        return pl.ds(pl.multiple_of(index * tok, tok), tok)

    smalls = [
        pltpu.make_async_copy(src, dst, in_sem.at[i])
        for i, (src, dst) in enumerate(
            (
                (ids_hbm, ids_ref),
                (q_hbm, q_ref),
                (kn_hbm, kn_ref),
                (vn_hbm, vn_ref),
                (kp_hbm, kp_ref),
                (vp_hbm, vp_ref),
                (order_hbm, order_ref),
                (res_hbm, res_ref),
                (gain_hbm, gain_ref),
                (router_hbm, router_ref),
            )
        )
    ]
    for small in smalls:
        small.start()

    barrier = pltpu.get_barrier_semaphore()
    for i in reversed(range(n_seq)):
        for j in reversed(range(n_rep)):
            if i or j:
                pl.semaphore_signal(
                    barrier,
                    inc=1,
                    device_id=dev(other(seq, i, n_seq), other(rep, j, n_rep)),
                    device_id_type=MESH,
                )

    loads = []
    for i, (src, dst) in enumerate(
        ((proj_hbm, wproj), (gate_hbm.at[0], wgate), (up_hbm.at[0], wup), (down_hbm.at[0], wdown))
    ):
        pieces = 1 if i == 0 else 4
        size = dst.shape[0] // pieces
        for j in range(pieces):
            span = pl.ds(j * size, size)
            load = pltpu.make_async_copy(src.at[span], dst.at[span], w_sem.at[i, j])
            load.start()
            loads.append(load)

    for small in smalls[:4]:
        small.wait()
    lane = lax.broadcasted_iota(jnp.int32, (tok, 128), 1)
    ids_f = ids_ref[...].astype(F32)
    diagonal = lax.broadcasted_iota(jnp.int32, (tok, tok), 0) == lax.broadcasted_iota(
        jnp.int32, (tok, tok), 1
    )
    picks = [
        jnp.sum(jnp.where(diagonal, ids_f[i : i + 1, :], 0.0), axis=1, keepdims=True)
        for i in range(2)
    ]
    idall[rows_of(seq), :] = jnp.where(lane == 0, picks[0], picks[1])
    qall[rows_of(seq), :] = q_ref[...]
    for j in range(n_rep):

        @pl.when(rep == j)
        def _():
            kcache[:, j * hd : (j + 1) * hd] = kn_ref[...]
            vcache[:, j * hd : (j + 1) * hd] = vn_ref[...]

    pl.semaphore_wait(barrier, n_seq * n_rep - 1)

    sends = []

    def send(copy):
        copy.start()
        sends.append(copy)

    for k in range(1, n_seq):
        to = other(seq, k, n_seq)
        mine = rows_of(seq)
        send(remote(q_ref, qall.at[mine], small_send.at[0, k], small_recv.at[0, seq], to, rep))
    for k in range(1, n_seq):
        to = other(seq, k, n_seq)
        mine = rows_of(seq)
        send(
            remote(idall.at[mine], idall.at[mine], small_send.at[1, k], small_recv.at[1, seq], to, rep)
        )

    for small in smalls[4:]:
        small.wait()
    own_pos = order_ref[seq] * tok + lax.broadcasted_iota(jnp.int32, (tok, tok), 1)
    bias = [
        jnp.where(
            own_pos <= order_ref[t] * tok + lax.broadcasted_iota(jnp.int32, (tok, tok), 0),
            0.0,
            -1e30,
        )
        for t in range(n_seq)
    ]
    bias = jnp.concatenate(bias * q_per, axis=0)

    for k in range(1, n_seq):
        frm = other(seq, k, n_seq)
        src = rows_of(frm)
        remote(q_ref, qall.at[src], small_send.at[0, k], small_recv.at[0, frm], frm, rep).wait_recv()

    scaling = 1.0 / math.sqrt(hd)
    queries = jnp.concatenate([qall[:, h * hd : (h + 1) * hd] for h in range(q_per)], axis=0)
    nt = (((1,), (1,)), ((), ()))
    s_past = lax.dot_general(queries, kp_ref[...], nt, preferred_element_type=F32) * scaling
    s_new = lax.dot_general(queries, kn_ref[...], nt, preferred_element_type=F32) * scaling + bias
    high = jnp.maximum(
        jnp.max(s_past, axis=1, keepdims=True), jnp.max(s_new, axis=1, keepdims=True)
    )
    w_past = jnp.exp(s_past - high)
    w_new = jnp.exp(s_new - high)
    total = jnp.sum(w_past, axis=1, keepdims=True) + jnp.sum(w_new, axis=1, keepdims=True)
    num = jnp.dot(w_past.astype(BF16), vp_ref[...], preferred_element_type=F32) + jnp.dot(
        w_new.astype(BF16), vn_ref[...], preferred_element_type=F32
    )
    rows = num.shape[0]
    stat_lane = lax.broadcasted_iota(jnp.int32, (rows, 128), 1)
    stats = jnp.where(stat_lane == 0, high, total)
    stat_send[...] = stats.T[:STAT_ROWS, :]
    num_send[...] = num.astype(BF16)

    stat_rows = pl.ds(pl.multiple_of(seq * STAT_ROWS, STAT_ROWS), STAT_ROWS)

    def partial_copies(k):
        to = same_core(k)
        return (
            remote(num_send, num_all.at[seq], num_ssem.at[0, k], num_rsem.at[0, seq], rep, to),
            remote(
                stat_send, stat_all.at[stat_rows], num_ssem.at[1, k], num_rsem.at[1, seq], rep, to
            ),
        )

    for k in range(1, chips):
        for copy in partial_copies(k):
            send(copy)

    @pl.when(seq != rep)
    def _():
        for copy in partial_copies(0):
            copy.start()

    @pl.when(seq == rep)
    def _():
        num_all[seq] = num_send[...]
        stat_all[stat_rows, :] = stat_send[...]

    for j in range(n_rep):

        @pl.when(rep == j)
        def _():
            cols = pl.ds(j * hd, hd)
            for k in range(1, n_rep):
                to = (j + k) % n_rep
                remote(
                    kn_ref, kcache.at[:, cols], small_send.at[2, k], small_recv.at[2, j], seq, to
                ).start()
                remote(
                    vn_ref, vcache.at[:, cols], small_send.at[3, k], small_recv.at[3, j], seq, to
                ).start()

    def wait_partial(frm):
        src_rows = pl.ds(pl.multiple_of(frm * STAT_ROWS, STAT_ROWS), STAT_ROWS)
        remote(
            num_send, num_all.at[frm], num_ssem.at[0, 0], num_rsem.at[0, frm], seq, rep
        ).wait_recv()
        remote(
            stat_send, stat_all.at[src_rows], num_ssem.at[1, 0], num_rsem.at[1, frm], seq, rep
        ).wait_recv()

    def handed(frm):
        src_rows = pl.ds(pl.multiple_of(frm * STAT_ROWS, STAT_ROWS), STAT_ROWS)
        return (
            remote(
                num_all.at[frm], num_all.at[frm], hand_ssem.at[0, frm], num_rsem.at[0, frm], seq, partner
            ),
            remote(
                stat_all.at[src_rows],
                stat_all.at[src_rows],
                hand_ssem.at[1, frm],
                num_rsem.at[1, frm],
                seq,
                partner,
            ),
        )

    first_core = lax.rem(seq, 2)

    @pl.when(core == first_core)
    def _():
        @pl.when(seq == rep)
        def _():
            for copy in handed(seq):
                copy.start()

        for k in range(1, n_seq):
            frm = other(seq, k, n_seq)
            wait_partial(frm)
            for copy in handed(frm):
                copy.start()

        @pl.when(seq != rep)
        def _():
            wait_partial(seq)
            for copy in handed(seq):
                copy.start()

    @pl.when(core != first_core)
    def _():
        for k in range(n_seq):
            wait_partial(other(seq, k, n_seq))

    @pl.when(seq != rep)
    def _():
        for copy in partial_copies(0):
            copy.wait_send()

    stat_cols = jnp.concatenate(
        [stat_all[...], jnp.zeros((128 - n_seq * STAT_ROWS, rows), F32)], axis=0
    ).T
    highs = [stat_cols[:, s * STAT_ROWS : s * STAT_ROWS + 1] for s in range(n_seq)]
    top = functools.reduce(jnp.maximum, highs)
    scales = [jnp.exp(h - top) for h in highs]
    full = sum(
        scales[s] * stat_cols[:, s * STAT_ROWS + 1 : s * STAT_ROWS + 2] for s in range(n_seq)
    )
    heads = sum(scales[s] * num_all[s].astype(F32) for s in range(n_seq)) / full
    heads = heads.astype(BF16)
    head_rows = jnp.concatenate([heads[h * toks : (h + 1) * toks] for h in range(q_per)], axis=1)
    loads[0].wait()
    part_send[...] = jnp.dot(head_rows, wproj[...], preferred_element_type=F32).astype(BF16)
    for k in range(1, n_seq):
        to = other(seq, k, n_seq)
        send(
            remote(
                part_send.at[rows_of(to)], part_all.at[seq], part_ssem.at[k], part_rsem.at[seq], to, rep
            )
        )
    projected = part_send[rows_of(seq), :].astype(F32)
    for k in range(1, n_seq):
        frm = other(seq, k, n_seq)
        remote(
            part_send.at[rows_of(frm)], part_all.at[frm], part_ssem.at[k], part_rsem.at[frm], frm, rep
        ).wait_recv()
        projected = projected + part_all[frm].astype(F32)
    attended = (res_ref[...].astype(F32) + projected).astype(BF16)
    att_out[...] = attended
    xall[rep, rows_of(seq), :] = attended

    def x_copy(r, s, slot, to_s, to_r):
        view = xall.at[r, rows_of(s)]
        return remote(view, view, x_ssem.at[slot[0], slot[1]], x_rsem.at[r, s], to_s, to_r)

    for k in range(1, n_seq):
        send(x_copy(rep, seq, (0, k), other(seq, k, n_seq), rep))
    def spread(frm, k):
        for j in range(1, chips):
            send(x_copy(rep, frm, (1 + j, k), seq, same_core(j)))
        send(x_copy(rep, frm, (1, k), seq, partner))

    spread(seq, 0)
    for k in range(1, n_seq):
        frm = other(seq, n_seq - k, n_seq)
        x_copy(rep, frm, (0, k), frm, rep).wait_recv()
        spread(frm, k)

    def quarter_wait(at):
        for k in range(n_seq):
            x_copy(at, other(seq, n_seq - k, n_seq), (1, k), seq, at).wait_recv()

    for load in loads[1:9]:
        load.wait()
    hidden_width = wgate.shape[1]
    chunk = min(512, hidden_width)

    def scaled_quarter(at):
        cols = pl.ds(pl.multiple_of(at * feat, feat), feat)
        part = xall[at].astype(F32)
        gained[...] = (part * gain_ref[:, cols]).astype(BF16)
        return jnp.sum(part * part, axis=1, keepdims=True)

    def products(at, cols):
        span = pl.ds(pl.multiple_of(at * feat, feat), feat)
        return (
            jnp.dot(gained[...], wgate[span, cols], preferred_element_type=F32),
            jnp.dot(gained[...], wup[span, cols], preferred_element_type=F32),
        )

    def add_quarter(at, start):
        for c in range(hidden_width // chunk):
            cols = pl.ds(c * chunk, chunk)
            gate, up = products(at, cols)
            if start:
                gate_acc[:, cols] = gate
                up_acc[:, cols] = up
            else:
                gate_acc[:, cols] += gate
                up_acc[:, cols] += up

    squares = scaled_quarter(rep)
    add_quarter(rep, True)
    quarter_wait(partner)
    squares = squares + scaled_quarter(partner)
    add_quarter(partner, False)
    for j in range(1, chips):
        at = same_core(j)
        quarter_wait(at)
        send(remote(xall.at[at], xall.at[at], pass_ssem.at[j], pass_rsem.at[j], seq, partner))
        squares = squares + scaled_quarter(at)
        add_quarter(at, False)
    for j in range(1, chips):
        at = other_core(j)
        remote(
            xall.at[at], xall.at[at], pass_ssem.at[j], pass_rsem.at[j], seq, partner
        ).wait_recv()
        squares = squares + scaled_quarter(at)
        if j < chips - 1:
            add_quarter(at, False)
    last = other_core(chips - 1)
    inverse = lax.rsqrt(squares / (feat * n_rep) + 1e-05)
    inverse_ref[...] = jnp.broadcast_to(inverse, (toks, 128))

    for c in range(hidden_width // chunk):
        cols = pl.ds(c * chunk, chunk)
        factor = inverse_ref[:, 0:1]
        gate, up = products(last, cols)
        gate = (gate_acc[:, cols] + gate) * factor
        up = (up_acc[:, cols] + up) * factor
        hidden[:, cols] = (gate * jax.nn.sigmoid(gate) * up).astype(BF16)

    for load in loads[9:]:
        load.wait()
    targets = [f(j) for j in range(1, chips) for f in (same_core, other_core)]
    targets = list(enumerate(targets + [partner], 1)) + [(0, rep)]
    for k, to in targets:
        cols = pl.ds(pl.multiple_of(to * feat, feat), feat)
        product = jnp.dot(hidden[...], wdown[:, cols], preferred_element_type=F32).astype(BF16)
        if k:
            ysend[k - 1] = product
            send(remote(ysend.at[k - 1], yall.at[rep], y_ssem.at[k], y_rsem.at[rep], seq, to))
        else:
            yall[rep] = product

    for k in range(1, n_seq):
        frm = other(seq, k, n_seq)
        src = rows_of(frm)
        remote(
            idall.at[src], idall.at[src], small_send.at[1, k], small_recv.at[1, frm], frm, rep
        ).wait_recv()
    experts = router_ref.shape[0]
    logits = [jnp.zeros((toks, 1), F32) for _ in range(experts)]
    for j in range(n_rep):
        cols = slice(j * feat, (j + 1) * feat)
        part = (xall[j].astype(F32) * gain_ref[:, cols] * inverse).astype(BF16).astype(F32)
        for e in range(experts):
            logits[e] = logits[e] + jnp.sum(part * router_ref[e : e + 1, cols], axis=1, keepdims=True)
    first = [(idall[:, 0:1] == float(e)).astype(F32) for e in range(experts)]
    second = [(idall[:, 1:2] == float(e)).astype(F32) for e in range(experts)]
    gap = sum(first[e] * logits[e] for e in range(experts)) - sum(
        second[e] * logits[e] for e in range(experts)
    )
    share = jax.nn.sigmoid(gap)
    shares = [share * first[e] + (1.0 - share) * second[e] for e in range(experts)]

    for k in range(1, n_rep):
        frm = other(rep, k, n_rep)
        remote(ysend.at[0], yall.at[frm], y_ssem.at[k], y_rsem.at[frm], seq, frm).wait_recv()
    mixture = sum(shares[j % experts] * yall[j].astype(F32) for j in range(n_rep))
    zsend[...] = mixture.astype(BF16)
    for k in range(1, n_seq):
        to = other(seq, k, n_seq)
        send(remote(zsend.at[rows_of(to)], zall.at[seq], z_ssem.at[k], z_rsem.at[seq], to, rep))
    for j in range(n_rep):

        @pl.when(rep != j)
        def _():
            cols = pl.ds(j * hd, hd)
            remote(
                kn_ref, kcache.at[:, cols], small_send.at[2, 0], small_recv.at[2, j], seq, rep
            ).wait_recv()
            remote(
                vn_ref, vcache.at[:, cols], small_send.at[3, 0], small_recv.at[3, j], seq, rep
            ).wait_recv()

    kc_out[...] = kcache[...]
    vc_out[...] = vcache[...]
    result = xall[rep, rows_of(seq), :].astype(F32) + zsend[rows_of(seq), :].astype(F32)
    for k in range(1, n_seq):
        frm = other(seq, k, n_seq)
        remote(
            zsend.at[rows_of(frm)], zall.at[frm], z_ssem.at[k], z_rsem.at[frm], frm, rep
        ).wait_recv()
        result = result + zall[frm].astype(F32)
    layer_out[...] = result.astype(BF16)

    for copy in sends:
        copy.wait_send()

    @pl.when(core == first_core)
    def _():
        for s in range(n_seq):
            for copy in handed(s):
                copy.wait_send()

    for k in range(1, n_rep):
        for which, src in ((2, kn_ref), (3, vn_ref)):
            remote(
                src,
                (kcache if which == 2 else vcache).at[:, pl.ds(0, hd)],
                small_send.at[which, k],
                small_recv.at[which, 0],
                seq,
                rep,
            ).wait_send()


def hand_over(*refs):
    sem = refs[8]
    copies = [pltpu.make_async_copy(refs[i], refs[4 + i], sem.at[i]) for i in range(4)]
    for copy in copies:
        copy.start()
    for copy in copies:
        copy.wait()


def fused_body(
    queries,
    keys_new,
    values_new,
    keys_past,
    values_past,
    block_order,
    residual,
    out_proj,
    norm_gain,
    router,
    w_gate,
    w_up,
    w_down,
    expert_ids,
):
    n_seq = lax.axis_size("seq")
    n_rep = lax.axis_size("rep")
    tok, width = queries.shape
    hd = keys_new.shape[1]
    toks = tok * n_seq
    rows = toks * (width // hd)
    feat = residual.shape[1]
    vmem = pl.BlockSpec(memory_space=pltpu.VMEM)
    hbm = pl.BlockSpec(memory_space=pl.ANY)
    dma = pltpu.SemaphoreType.DMA
    cache = (tok, hd * n_rep)
    outs = pl.pallas_call(
        functools.partial(fused_kernel, n_seq, n_rep),
        out_shape=(
            pltpu.VMEM((tok, feat), BF16),
            pltpu.VMEM((tok, feat), BF16),
            pltpu.VMEM(cache, BF16),
            pltpu.VMEM(cache, BF16),
        ),
        in_specs=[hbm] * 14,
        out_specs=(vmem,) * 4,
        scratch_shapes=[
            pltpu.SMEM(block_order.shape, jnp.int32),
            pltpu.VMEM(queries.shape, BF16),
            pltpu.VMEM(keys_new.shape, BF16),
            pltpu.VMEM(values_new.shape, BF16),
            pltpu.VMEM(keys_past.shape, BF16),
            pltpu.VMEM(values_past.shape, BF16),
            pltpu.VMEM(residual.shape, BF16),
            pltpu.VMEM((1, norm_gain.shape[0]), F32),
            pltpu.VMEM(router.shape[::-1], F32),
            pltpu.VMEM(expert_ids.shape[::-1], jnp.int32),
            dma((10,)),
            pltpu.VMEM(out_proj.shape, BF16),
            pltpu.VMEM(w_gate.shape[1:], BF16),
            pltpu.VMEM(w_up.shape[1:], BF16),
            pltpu.VMEM(w_down.shape[1:], BF16),
            pltpu.VMEM((toks, width), BF16),
            pltpu.VMEM((toks, 128), F32),
            pltpu.VMEM(cache, BF16),
            pltpu.VMEM(cache, BF16),
            pltpu.VMEM((rows, hd), BF16),
            pltpu.VMEM((STAT_ROWS, rows), F32),
            pltpu.VMEM((n_seq, rows, hd), BF16),
            pltpu.VMEM((n_seq * STAT_ROWS, rows), F32),
            pltpu.VMEM((toks, feat), BF16),
            pltpu.VMEM((n_seq, tok, feat), BF16),
            pltpu.VMEM((n_rep, toks, feat), BF16),
            pltpu.VMEM((toks, feat), BF16),
            pltpu.VMEM((toks, w_gate.shape[2]), F32),
            pltpu.VMEM((toks, w_gate.shape[2]), F32),
            pltpu.VMEM((toks, 128), F32),
            pltpu.VMEM((toks, w_gate.shape[2]), BF16),
            pltpu.VMEM((n_rep - 1, toks, feat), BF16),
            pltpu.VMEM((n_rep, toks, feat), BF16),
            pltpu.VMEM((toks, feat), BF16),
            pltpu.VMEM((n_seq, tok, feat), BF16),
            dma((4, 4)),
            dma((4, max(n_seq, n_rep))),
            dma((4, max(n_seq, n_rep))),
            dma((2, n_rep)),
            dma((2, n_seq)),
            dma((2, n_seq)),
            dma((n_rep,)),
            dma((n_rep,)),
            dma((n_seq,)),
            dma((n_seq,)),
            dma((n_rep, n_seq)),
            dma((n_rep, n_seq)),
            dma((n_rep,)),
            dma((n_rep,)),
            dma((n_seq,)),
            dma((n_seq,)),
        ],
        compiler_params=pltpu.CompilerParams(
            collective_id=0, has_side_effects=True, vmem_limit_bytes=62 * 1024 * 1024
        ),
    )(
        block_order,
        queries,
        keys_new,
        values_new,
        keys_past,
        values_past,
        residual,
        norm_gain.reshape(1, -1),
        router.T,
        expert_ids.T,
        out_proj,
        w_gate,
        w_up,
        w_down,
    )
    return pl.pallas_call(
        hand_over,
        out_shape=tuple(jax.ShapeDtypeStruct(out.shape, out.dtype) for out in outs),
        in_specs=[hbm] * 4,
        out_specs=(hbm,) * 4,
        scratch_shapes=[dma((4,))],
    )(*[pltpu.with_memory_space_constraint(out, pltpu.VMEM) for out in outs])


def body(*arrays):
    queries, out_proj = arrays[0], arrays[7]
    n_seq, n_rep = lax.axis_size("seq"), lax.axis_size("rep")
    held = 2 * sum(math.prod(array.shape) for array in arrays[10:13])
    fits = held <= 50 * 1024 * 1024 and n_seq * STAT_ROWS <= 128 and n_seq == n_rep and n_rep % 2 == 0 and n_rep > 2
    if fits and out_proj.shape[0] == queries.shape[1]:
        return fused_body(*arrays)
    return plain_body(*arrays)


def solution(mesh):
    in_specs = (
        P(("groups", "seq"), "rep"),
        P(("groups", "seq"), "rep"),
        P(("groups", "seq"), "rep"),
        P(("groups", "seq"), "rep"),
        P(("groups", "seq"), "rep"),
        P("groups"),
        P(("groups", "seq"), "rep"),
        P("seq", "rep"),
        P(),
        P(),
        P("rep", None, "seq"),
        P("rep", None, "seq"),
        P("rep", "seq", None),
        P(("groups", "seq"), None),
    )
    out_specs = (
        P(("groups", "seq"), "rep"),
        P(("groups", "seq"), "rep"),
        P(("groups", "seq"), None),
        P(("groups", "seq"), None),
    )
    return jax.shard_map(body, mesh=mesh, in_specs=in_specs, out_specs=out_specs, check_vma=False)
```

```python
import functools
import math

import jax
import jax.numpy as jnp
from jax import lax
from jax.experimental import pallas as pl
from jax.experimental.pallas import tpu as pltpu
from jax.sharding import PartitionSpec as P

EXPERTS = 4
CAP = 12


def block_lookup(owners, block_order):
    width = block_order.shape[0]
    hits = owners[:, None] == jnp.arange(width, dtype=jnp.int32)[None, :]
    return jnp.sum(jnp.where(hits, block_order[None, :], 0), axis=1)


def plain_body(
    queries,
    keys_new,
    values_new,
    keys_past,
    values_past,
    block_order,
    residual,
    out_proj,
    norm_gain,
    router,
    w_gate,
    w_up,
    w_down,
    expert_ids,
):
    seq_index = lax.axis_index("seq")
    rep_index = lax.axis_index("rep")
    rep_count = lax.axis_size("rep")
    tok_count = queries.shape[0]
    head_dim = keys_new.shape[1]
    q_per = queries.shape[1] // head_dim
    past_len = keys_past.shape[0]
    key_span = past_len + tok_count
    row_total = tok_count * q_per
    my_block = block_lookup(jnp.full((1,), seq_index, jnp.int32), block_order)[0]
    scaling = 1.0 / math.sqrt(head_dim)
    query_rows = queries.reshape(row_total, head_dim)
    query_pos = my_block * tok_count + jnp.arange(row_total, dtype=jnp.int32) // q_per
    keys_local = jnp.concatenate([keys_past, keys_new], axis=0)
    values_local = jnp.concatenate([values_past, values_new], axis=0)
    running = jnp.full((row_total,), -1e30, jnp.float32)
    key_piece = lax.all_gather(keys_local, "seq", axis=0, tiled=True)
    value_piece = lax.all_gather(values_local, "seq", axis=0, tiled=True)
    row_count = key_piece.shape[0]
    key_index = jnp.arange(row_count, dtype=jnp.int32)
    key_owner = key_index // key_span
    offset = key_index % key_span
    key_pos = block_lookup(key_owner, block_order) * tok_count + offset - past_len
    visible = (offset < past_len)[None, :] | (key_pos[None, :] <= query_pos[:, None])
    scores = jnp.dot(query_rows, key_piece.T, preferred_element_type=jnp.float32) * scaling
    highest = jnp.maximum(running, jnp.max(jnp.where(visible, scores, -1e30), axis=1))
    weights = jnp.where(visible, jnp.exp(scores - highest[:, None]), 0.0)
    totals = jnp.sum(weights, axis=1)
    numerator = jnp.dot(
        weights.astype(jnp.bfloat16), value_piece, preferred_element_type=jnp.float32
    )
    running, totals, numerator = (highest, totals, numerator)
    attn_local = (
        (numerator / totals[:, None]).reshape(tok_count, q_per * head_dim).astype(jnp.bfloat16)
    )
    attn_full, keys_cache, values_cache = (
        lax.all_gather(attn_local, "rep", axis=1, tiled=True),
        lax.all_gather(keys_new, "rep", axis=1, tiled=True),
        lax.all_gather(values_new, "rep", axis=1, tiled=True),
    )
    head_rows = lax.all_to_all(attn_full, "seq", split_axis=1, concat_axis=0, tiled=True)
    projected = lax.psum_scatter(
        jnp.dot(head_rows, out_proj, preferred_element_type=jnp.float32).astype(jnp.bfloat16),
        "seq",
        scatter_dimension=0,
        tiled=True,
    ).astype(jnp.float32)
    attended = (residual.astype(jnp.float32) + projected).astype(jnp.bfloat16)
    full_rows = lax.all_gather(attended, "rep", axis=1, tiled=True)
    features = full_rows.astype(jnp.float32)
    mean_square = jnp.mean(features * features, axis=1, keepdims=True)
    normed = (features * norm_gain[None, :] * lax.rsqrt(mean_square + 1e-05)).astype(jnp.bfloat16)
    logits = jnp.dot(normed.astype(jnp.float32), router, precision=lax.Precision.HIGHEST)
    expert_range = jnp.arange(EXPERTS, dtype=jnp.int32)
    first_pick = (expert_ids[:, 0:1] == expert_range[None, :]).astype(jnp.float32)
    second_pick = (expert_ids[:, 1:2] == expert_range[None, :]).astype(jnp.float32)
    share_first = jax.nn.sigmoid(
        jnp.sum(first_pick * logits, axis=1) - jnp.sum(second_pick * logits, axis=1)
    )
    token_share = share_first[:, None] * first_pick + (1.0 - share_first)[:, None] * second_pick
    member = first_pick + second_pick
    ranking = jnp.cumsum(member, axis=0) - member
    slot_range = jnp.arange(CAP, dtype=jnp.float32)
    selection = member.T[:, None, :] * (ranking.T[:, None, :] == slot_range[None, :, None]).astype(
        jnp.float32
    )
    mine_mask = (expert_range == rep_index % EXPERTS).astype(jnp.float32)
    my_selection = jnp.einsum("e,ejt->jt", mine_mask, selection)
    slot_rows = jnp.dot(
        my_selection.astype(jnp.bfloat16), normed, preferred_element_type=jnp.float32
    ).astype(jnp.bfloat16)
    gate_local = w_gate[0]
    up_local = w_up[0]
    down_local = w_down[0]
    piece = lax.all_gather(slot_rows, "seq", axis=0, tiled=True)
    gate_part = jnp.dot(piece, gate_local, preferred_element_type=jnp.float32)
    up_part = jnp.dot(piece, up_local, preferred_element_type=jnp.float32)
    hidden_slots = (jax.nn.silu(gate_part) * up_part).astype(jnp.bfloat16)
    expert_part = lax.psum_scatter(
        jnp.dot(hidden_slots, down_local, preferred_element_type=jnp.float32).astype(jnp.bfloat16),
        "seq",
        scatter_dimension=0,
        tiled=True,
    ).astype(jnp.float32)
    returned = lax.all_to_all(
        expert_part.astype(jnp.bfloat16), "rep", split_axis=1, concat_axis=0, tiled=True
    ).astype(expert_part.dtype)
    source_expert = jnp.arange(rep_count, dtype=jnp.int32) % EXPERTS
    source_pick = (source_expert[:, None] == expert_range[None, :]).astype(jnp.float32)
    combine = jnp.einsum("re,ejt,te->trj", source_pick, selection, token_share).reshape(
        tok_count, rep_count * CAP
    )
    moe_slice = jnp.dot(combine, returned, precision=lax.Precision.HIGHEST)
    layer_out = (attended.astype(jnp.float32) + moe_slice).astype(jnp.bfloat16)
    return (attended, layer_out, keys_cache, values_cache)


MESH = pl.DeviceIdType.MESH
HALF = 2
F32 = jnp.float32
BF16 = jnp.bfloat16


def fused_kernel(
    n_seq,
    n_rep,
    order_hbm,
    q_hbm,
    kn_hbm,
    vn_hbm,
    kp_hbm,
    vp_hbm,
    res_hbm,
    gain_hbm,
    router_hbm,
    ids_hbm,
    proj_hbm,
    gate_hbm,
    up_hbm,
    down_hbm,
    att_out,
    layer_out,
    kc_out,
    vc_out,
    order_ref,
    q_ref,
    kn_ref,
    vn_ref,
    kp_ref,
    vp_ref,
    res_ref,
    gain_ref,
    router_ref,
    ids_ref,
    in_sem,
    wproj,
    wgate,
    wup,
    wdown,
    qall,
    idall,
    kcache,
    vcache,
    num_send,
    num_all,
    head_send,
    head_all,
    res_all,
    part_send,
    part_all,
    xall,
    gained,
    router_split,
    gate_acc,
    up_acc,
    hidden,
    ysend,
    yall,
    psend,
    fin_all,
    w_sem,
    q_rsem,
    side_rsem,
    cache_rsem,
    cache_ssem,
    num_rsem,
    head_ssem,
    head_rsem,
    part_rsem,
    x_rsem,
    y_rsem,
    z_rsem,
    send_sem,
):
    group = lax.axis_index("groups")
    seq = lax.axis_index("seq")
    rep = lax.axis_index("rep")
    tok, width = q_ref.shape
    hd = kn_ref.shape[1]
    q_per = width // hd
    toks = tok * n_seq
    feat = res_ref.shape[1]
    slab = feat // n_seq
    stat_rows = num_send.shape[1] - tok * q_per

    chips = n_rep // 2
    chip, core = rep // 2, lax.rem(rep, 2)
    partner = chip * 2 + 1 - core

    def same_core(step):
        return lax.rem(chip + step, chips) * 2 + core

    def other_core(step):
        return lax.rem(chip + step, chips) * 2 + 1 - core

    def dev(s, r):
        return {"groups": group, "seq": s, "rep": r}

    def other(index, step, size):
        return lax.rem(index + step, size)

    def remote(src, dst, ssem, rsem, s, r):
        return pltpu.make_async_remote_copy(
            src_ref=src,
            dst_ref=dst,
            send_sem=ssem,
            recv_sem=rsem,
            device_id=dev(s, r),
            device_id_type=MESH,
        )

    def rows_of(index):
        return pl.ds(pl.multiple_of(index * tok, tok), tok)

    def split_terms(rest):
        terms = []
        for _ in range(3):
            terms.append(rest.astype(BF16).astype(F32))
            rest = rest - terms[-1]
        return terms

    def size_of(ref):
        return math.prod(ref.shape) * ref.dtype.itemsize

    def wait_all(sem, size):
        tiles = size // (16 * 128 * 2)
        wide = max(w for w in range(1, wgate.shape[1] // 128 + 1) if tiles % w == 0)
        span = wgate.at[pl.ds(0, tiles // wide * 16), pl.ds(0, wide * 128)]
        pltpu.make_async_copy(span, span, sem).wait()

    def slab_of(index):
        return pl.ds(pl.multiple_of(index * slab, slab), slab)

    def per_seq(rows):
        return [sum(jnp.where(seq == s, rows[s][k], 0) for s in range(n_seq)) for k in range(n_seq - 1)]

    def others(s):
        return [t for t in range(n_seq) if t != s]

    far_first = per_seq([sorted(others(s), key=lambda t: -abs(t - s)) for s in range(n_seq)])
    arrivals = per_seq(
        [
            sorted(others(s), key=lambda f: (abs(f - s), f if 2 * s < n_seq else -f))
            for s in range(n_seq)
        ]
    )

    smalls = [
        pltpu.make_async_copy(src, dst, in_sem.at[(0, 1, 2, 2, 3, 3, 4, 5, 6, 7)[i]])
        for i, (src, dst) in enumerate(
            (
                (ids_hbm, ids_ref),
                (q_hbm, q_ref),
                (kn_hbm, kn_ref),
                (vn_hbm, vn_ref),
                (kp_hbm, kp_ref),
                (vp_hbm, vp_ref),
                (order_hbm, order_ref),
                (res_hbm, res_ref),
                (gain_hbm, gain_ref),
                (router_hbm, router_ref),
            )
        )
    ]
    for small in smalls:
        small.start()

    barrier = pltpu.get_barrier_semaphore()
    for i in reversed(range(n_seq)):
        for j in reversed(range(n_rep)):
            if i or j:
                pl.semaphore_signal(
                    barrier,
                    inc=1,
                    device_id=dev(other(seq, i, n_seq), other(rep, j, n_rep)),
                    device_id_type=MESH,
                )

    loads = []
    for i, (src, dst) in enumerate(
        ((proj_hbm, wproj), (gate_hbm.at[0], wgate), (up_hbm.at[0], wup), (down_hbm.at[0], wdown))
    ):
        pieces = 1 if i == 0 else 4
        size = dst.shape[0] // pieces
        for j in range(pieces):
            span = pl.ds(j * size, size)
            pltpu.make_async_copy(src.at[span], dst.at[span], w_sem.at[i]).start()
        loads.append(pltpu.make_async_copy(src, dst, w_sem.at[i]))

    smalls[0].wait()
    smalls[1].wait()
    wait_all(in_sem.at[2], 2 * size_of(kn_ref))
    lane = lax.broadcasted_iota(jnp.int32, (tok, 128), 1)
    ids_f = ids_ref[...].astype(F32)
    diagonal = lax.broadcasted_iota(jnp.int32, (tok, tok), 0) == lax.broadcasted_iota(
        jnp.int32, (tok, tok), 1
    )
    picks = [
        jnp.sum(jnp.where(diagonal, ids_f[i : i + 1, :], 0.0), axis=1, keepdims=True)
        for i in range(2)
    ]
    idall[rows_of(seq), :] = jnp.where(lane == 0, picks[0], picks[1])
    qall[rows_of(seq), :] = q_ref[...]
    for j in range(n_rep):

        @pl.when(rep == j)
        def _():
            kcache[:, j * hd : (j + 1) * hd] = kn_ref[...]
            vcache[:, j * hd : (j + 1) * hd] = vn_ref[...]

    pl.semaphore_wait(barrier, n_seq * n_rep - 1)

    sent = [0]

    def send(ref, *rest):
        sent[0] += size_of(ref)
        remote(ref, rest[0], send_sem, *rest[1:]).start()

    mine = rows_of(seq)
    for to in far_first:
        send(q_ref, qall.at[mine], q_rsem, to, rep)

    experts = router_ref.shape[0]
    wait_all(in_sem.at[3], 2 * size_of(kp_ref))
    for small in smalls[6:]:
        small.wait()
    own_pos = order_ref[seq] * tok + lax.broadcasted_iota(jnp.int32, (tok, tok), 1)
    bias = [
        jnp.where(
            own_pos <= order_ref[t] * tok + lax.broadcasted_iota(jnp.int32, (tok, tok), 0),
            0.0,
            -1e30,
        )
        for t in range(n_seq)
    ]
    bias = jnp.concatenate([block for block in bias for _ in range(q_per)], axis=0)

    terms = split_terms(router_ref[...])
    terms.append(jnp.zeros((router_split.shape[0] - 3 * experts, router_ref.shape[1]), F32))
    router_split[...] = jnp.concatenate(terms, axis=0).astype(BF16)
    for to in far_first:
        send(res_ref.at[:, slab_of(to)], res_all.at[mine], side_rsem, to, rep)
        send(idall.at[mine], idall.at[mine], side_rsem, to, rep)
    res_all[mine, :] = res_ref[:, slab_of(seq)]

    wait_all(q_rsem, (n_seq - 1) * size_of(q_ref))

    scaling = 1.0 / math.sqrt(hd)
    queries = jnp.concatenate(
        [
            qall[t * tok : (t + 1) * tok, h * hd : (h + 1) * hd]
            for t in range(n_seq)
            for h in range(q_per)
        ],
        axis=0,
    )
    nt = (((1,), (1,)), ((), ()))
    s_past = lax.dot_general(queries, kp_ref[...], nt, preferred_element_type=F32) * scaling
    s_new = lax.dot_general(queries, kn_ref[...], nt, preferred_element_type=F32) * scaling + bias
    high = jnp.maximum(
        jnp.max(s_past, axis=1, keepdims=True), jnp.max(s_new, axis=1, keepdims=True)
    )
    w_past = jnp.exp(s_past - high)
    w_new = jnp.exp(s_new - high)
    total = jnp.sum(w_past, axis=1, keepdims=True) + jnp.sum(w_new, axis=1, keepdims=True)
    num = jnp.dot(w_past.astype(BF16), vp_ref[...], preferred_element_type=F32) + jnp.dot(
        w_new.astype(BF16), vn_ref[...], preferred_element_type=F32
    )
    rows = num.shape[0]
    stat_lane = lax.broadcasted_iota(jnp.int32, (rows, 128), 1)
    stats = jnp.where(stat_lane == 0, high, total).T
    span = rows // n_seq
    for t in range(n_seq):
        line = jnp.concatenate([stats[i : i + 1, t * span : (t + 1) * span] for i in range(2)], axis=1)
        coded = split_terms(line) + [jnp.zeros((stat_rows - 3, 2 * span), F32)]
        num_send[t, :span, :] = num[t * span : (t + 1) * span].astype(BF16)
        num_send[t, span:, :] = jnp.concatenate(coded, axis=0).astype(BF16)

    for to in far_first:
        send(num_send.at[to], num_all.at[seq], num_rsem, to, rep)
    num_all[seq] = num_send[seq]
    for j in range(n_rep):

        @pl.when(rep == j)
        def _():
            cols = pl.ds(j * hd, hd)
            for k in range(1, n_rep):
                to = (j + k) % n_rep
                remote(kn_ref, kcache.at[:, cols], cache_ssem, cache_rsem, seq, to).start()
                remote(vn_ref, vcache.at[:, cols], cache_ssem, cache_rsem, seq, to).start()

    wait_all(num_rsem, (n_seq - 1) * size_of(num_send.at[0]))

    lines = []
    for i in range(n_seq):
        coded = num_all[i, span:, :].astype(F32)
        lines.append(coded[0:1] + coded[1:2] + coded[2:3])
    lines.append(jnp.zeros((128 - n_seq, 2 * span), F32))
    stat_cols = jnp.concatenate(lines, axis=0).T
    highs = [stat_cols[:span, i : i + 1] for i in range(n_seq)]
    top = functools.reduce(jnp.maximum, highs)
    scales = [jnp.exp(h - top) for h in highs]
    full = sum(scales[i] * stat_cols[span:, i : i + 1] for i in range(n_seq))
    heads = sum(scales[i] * num_all[i, :span, :].astype(F32) for i in range(n_seq)) / full
    head_send[...] = heads.astype(BF16)

    def head_copy(to):
        return remote(head_send, head_all.at[seq], head_ssem, head_rsem, rep, to)

    for j in range(1, chips):
        send(head_send, head_all.at[seq], head_rsem, rep, same_core(j))
        send(head_send, head_all.at[seq], head_rsem, rep, other_core(j))

    @pl.when(seq != rep)
    def _():
        head_copy(rep).start()

    send(head_send, head_all.at[seq], head_rsem, rep, partner)

    @pl.when(seq == rep)
    def _():
        head_all[seq] = head_send[...]
        wait_all(head_rsem, (n_seq - 1) * size_of(head_send))

    @pl.when(seq != rep)
    def _():
        wait_all(head_rsem, n_seq * size_of(head_send))
        head_copy(rep).wait_send()

    head_rows = jnp.concatenate(
        [
            jnp.concatenate([head_all[t, h * tok : (h + 1) * tok, :] for t in range(n_seq)], axis=0)
            for h in range(q_per)
        ],
        axis=1,
    )
    loads[0].wait()
    wait_all(side_rsem, (n_seq - 1) * (tok * slab * 2 + tok * 128 * 4))
    for k, to in enumerate(far_first):
        part_send[k] = jnp.dot(
            head_rows, wproj[:, slab_of(to)], preferred_element_type=F32
        ).astype(BF16)
        send(part_send.at[k], part_all.at[seq], part_rsem, to, rep)
    summed = jnp.dot(head_rows, wproj[:, slab_of(seq)], preferred_element_type=F32)
    summed = summed.astype(BF16).astype(F32)
    wait_all(part_rsem, (n_seq - 1) * toks * slab * 2)
    for frm in arrivals:
        summed = summed + part_all[frm].astype(F32)
    xall[rep, seq] = (res_all[...].astype(F32) + summed).astype(BF16)

    def x_send(r, s, to_s, to_r):
        view = xall.at[r, s]
        send(view, view, x_rsem.at[r, s], to_s, to_r)

    def arrive(r, s):
        view = xall.at[r, s]
        remote(view, view, send_sem, x_rsem.at[r, s], seq, r).wait_recv()

    def spread(s, direct):
        for j in range(1, chips):
            x_send(rep, s, seq, same_core(j))
            if direct:
                x_send(rep, s, seq, other_core(j))
        x_send(rep, s, seq, partner)

    def from_seq(k):
        arrive(rep, arrivals[k])
        spread(arrivals[k], k > 0)

    def from_chip(s):
        for j in range(1, chips):
            arrive(same_core(j), s)
            x_send(same_core(j), s, seq, partner)

    spread(seq, False)
    for to in reversed(far_first):
        x_send(rep, seq, to, rep)
    hidden_width = wgate.shape[1]
    chunk = min(512, hidden_width)
    squares = [jnp.zeros((toks, 128), F32)]
    logits = [jnp.zeros((toks, router_split.shape[0]), F32)]

    def prepare(slots):
        for i, (r, s) in enumerate(slots):
            cols = pl.ds(pl.multiple_of(r * feat + s * slab, slab), slab)
            part = xall[r, s].astype(F32)
            squared = part * part
            for j in range(slab // 128):
                squares[0] = squares[0] + squared[:, j * 128 : (j + 1) * 128]
            scaled = (part * gain_ref[:, cols]).astype(BF16)
            gained[:, i * slab : (i + 1) * slab] = scaled
            logits[0] = logits[0] + lax.dot_general(
                scaled, router_split[:, cols], nt, preferred_element_type=F32
            )

    def products(slots, cols):
        total = None
        for i, (r, s) in enumerate(slots):
            span = pl.ds(pl.multiple_of(r * feat + s * slab, slab), slab)
            block = gained[:, i * slab : (i + 1) * slab]
            pair = (
                jnp.dot(block, wgate[span, cols], preferred_element_type=F32),
                jnp.dot(block, wup[span, cols], preferred_element_type=F32),
            )
            total = pair if total is None else (total[0] + pair[0], total[1] + pair[1])
        return total

    def add_slots(slots, start=False):
        prepare(slots)
        for c in range(hidden_width // chunk):
            cols = pl.ds(c * chunk, chunk)
            gate, up = products(slots, cols)
            if start:
                gate_acc[:, cols] = gate
                up_acc[:, cols] = up
            else:
                gate_acc[:, cols] += gate
                up_acc[:, cols] += up

    for load in loads[1:3]:
        load.wait()
    arrive(partner, seq)
    add_slots([(rep, seq), (partner, seq)], True)
    from_seq(0)
    from_chip(seq)
    add_slots([(rep, arrivals[0]), (same_core(1), seq)])
    for k in range(1, n_seq - 1):
        from_seq(k)
    att_out[...] = jnp.concatenate([xall[rep, t, mine] for t in range(n_seq)], axis=1)
    arrive(partner, arrivals[0])
    arrive(other_core(1), seq)
    add_slots([(partner, arrivals[0]), (other_core(1), seq)])
    from_chip(arrivals[0])
    rest = arrivals[1:]
    add_slots([(rep, s) for s in rest])
    for s in rest:
        arrive(partner, s)
    add_slots([(partner, s) for s in rest])
    for s in rest[:-1]:
        arrive(same_core(1), s)
    add_slots([(same_core(1), s) for s in arrivals[:-1]])
    for s in arrivals[:-1]:
        arrive(other_core(1), s)
    add_slots([(other_core(1), s) for s in arrivals[:-1]])
    final = [(same_core(1), arrivals[-1]), (other_core(1), arrivals[-1])]
    for slot in final:
        arrive(*slot)
    prepare(final)
    square = jnp.sum(squares[0], axis=1, keepdims=True)
    inverse = lax.rsqrt(square / (feat * n_rep) + 1e-05)
    for c in range(hidden_width // chunk):
        cols = pl.ds(c * chunk, chunk)
        gate, up = products(final, cols)
        gate = (gate_acc[:, cols] + gate) * inverse
        up = (up_acc[:, cols] + up) * inverse
        hidden[:, cols] = (gate * jax.nn.sigmoid(gate) * up).astype(BF16)

    columns = [
        sum(logits[0][:, i * experts + e : i * experts + e + 1] for i in range(3)) * inverse
        for e in range(experts)
    ]
    first = [(idall[:, 0:1] == float(e)).astype(F32) for e in range(experts)]
    second = [(idall[:, 1:2] == float(e)).astype(F32) for e in range(experts)]
    gap = sum(first[e] * columns[e] for e in range(experts)) - sum(
        second[e] * columns[e] for e in range(experts)
    )
    share = jax.nn.sigmoid(gap)
    mine_first = (idall[:, 0:1] == (rep % experts).astype(F32)).astype(F32)
    mine_second = (idall[:, 1:2] == (rep % experts).astype(F32)).astype(F32)
    weight = share * mine_first + (1.0 - share) * mine_second

    loads[3].wait()
    half = feat // HALF

    def weighted(to_chip, to_core, h):
        start = (to_chip * 2 + to_core) * feat + h * half
        cols = pl.ds(pl.multiple_of(start, half), half)
        product = jnp.dot(hidden[...], wdown[:, cols], preferred_element_type=F32)
        return product * weight

    def y_wait(j, h):
        remote(ysend.at[j, h], yall.at[j, h], send_sem, y_rsem.at[j, h], seq, partner).wait_recv()

    def to_partner(j, h, product):
        ysend[j, h] = product.astype(BF16)
        send(ysend.at[j, h], yall.at[j, h], y_rsem.at[j, h], seq, partner)

    def to_owner(j, h, product):
        y_wait(j, h)
        psend[j, h] = (product + yall[j, h].astype(F32)).astype(BF16)
        owner = lax.rem(chip + j, chips) * 2 + core
        for to in far_first + [seq] * min(j, 1):
            place = fin_all.at[seq, chip, :, pl.ds(h * half, half)]
            send(psend.at[j, h, rows_of(to)], place, z_rsem.at[seq, chip], to, owner)

    far = range(1, chips)
    steps = [(j, h, True) for j in far for h in range(HALF)] + [(0, 0, True)]
    steps += [(j, h, False) for j in far for h in range(HALF)]
    steps += [(0, h, True) for h in range(1, HALF)] + [(0, h, False) for h in range(HALF)]
    held = None
    for j, h, cross in steps:
        product = weighted(lax.rem(chip + j, chips), 1 - core if cross else core, h)
        if held is not None:
            held()
        held = functools.partial(to_partner if cross else to_owner, j, h, product)
    held()

    wait_all(cache_rsem, 2 * (n_rep - 1) * size_of(kn_ref))
    kc_out[...] = kcache[...]
    vc_out[...] = vcache[...]
    wait_all(cache_ssem, 2 * (n_rep - 1) * size_of(kn_ref))
    wait_all(send_sem, sent[0])

    own = jnp.concatenate([psend[0, h, mine] for h in range(HALF)], axis=1)
    result = att_out[...].astype(F32) + own.astype(F32)
    for frm_s, frm_chip in [(seq, lax.rem(chip + j, chips)) for j in range(1, chips)] + [
        (s, lax.rem(chip + j, chips)) for s in arrivals for j in range(chips)
    ]:
        place = fin_all.at[frm_s, frm_chip]
        remote(place, place, send_sem, z_rsem.at[frm_s, frm_chip], frm_s, rep).wait_recv()
        result = result + fin_all[frm_s, frm_chip].astype(F32)
    layer_out[...] = result.astype(BF16)


def hand_over(*refs):
    sem = refs[8]
    copies = [pltpu.make_async_copy(refs[i], refs[4 + i], sem.at[i]) for i in range(4)]
    for copy in copies:
        copy.start()
    for copy in copies:
        copy.wait()


def fused_body(
    queries,
    keys_new,
    values_new,
    keys_past,
    values_past,
    block_order,
    residual,
    out_proj,
    norm_gain,
    router,
    w_gate,
    w_up,
    w_down,
    expert_ids,
):
    n_seq = lax.axis_size("seq")
    n_rep = lax.axis_size("rep")
    tok, width = queries.shape
    hd = keys_new.shape[1]
    toks = tok * n_seq
    rows = toks * (width // hd)
    feat = residual.shape[1]
    slab = feat // n_seq
    chips = n_rep // 2
    vmem = pl.BlockSpec(memory_space=pltpu.VMEM)
    hbm = pl.BlockSpec(memory_space=pl.ANY)
    dma = pltpu.SemaphoreType.DMA
    cache = (tok, hd * n_rep)
    outs = pl.pallas_call(
        functools.partial(fused_kernel, n_seq, n_rep),
        out_shape=(
            pltpu.VMEM((tok, feat), BF16),
            pltpu.VMEM((tok, feat), BF16),
            pltpu.VMEM(cache, BF16),
            pltpu.VMEM(cache, BF16),
        ),
        in_specs=[hbm] * 14,
        out_specs=(vmem,) * 4,
        scratch_shapes=[
            pltpu.SMEM(block_order.shape, jnp.int32),
            pltpu.VMEM(queries.shape, BF16),
            pltpu.VMEM(keys_new.shape, BF16),
            pltpu.VMEM(values_new.shape, BF16),
            pltpu.VMEM(keys_past.shape, BF16),
            pltpu.VMEM(values_past.shape, BF16),
            pltpu.VMEM(residual.shape, BF16),
            pltpu.VMEM((1, norm_gain.shape[0]), F32),
            pltpu.VMEM(router.shape[::-1], F32),
            pltpu.VMEM(expert_ids.shape[::-1], jnp.int32),
            dma((9,)),
            pltpu.VMEM(out_proj.shape, BF16),
            pltpu.VMEM(w_gate.shape[1:], BF16),
            pltpu.VMEM(w_up.shape[1:], BF16),
            pltpu.VMEM(w_down.shape[1:], BF16),
            pltpu.VMEM((toks, width), BF16),
            pltpu.VMEM((toks, 128), F32),
            pltpu.VMEM(cache, BF16),
            pltpu.VMEM(cache, BF16),
            pltpu.VMEM((n_seq, rows // n_seq + 16, hd), BF16),
            pltpu.VMEM((n_seq, rows // n_seq + 16, hd), BF16),
            pltpu.VMEM((rows // n_seq, hd), BF16),
            pltpu.VMEM((n_seq, rows // n_seq, hd), BF16),
            pltpu.VMEM((toks, slab), BF16),
            pltpu.VMEM((n_seq - 1, toks, slab), BF16),
            pltpu.VMEM((n_seq, toks, slab), BF16),
            pltpu.VMEM((n_rep, n_seq, toks, slab), BF16),
            pltpu.VMEM((toks, (n_seq - 2) * slab), BF16),
            pltpu.VMEM((16, norm_gain.shape[0]), BF16),
            pltpu.VMEM((toks, w_gate.shape[2]), F32),
            pltpu.VMEM((toks, w_gate.shape[2]), F32),
            pltpu.VMEM((toks, w_gate.shape[2]), BF16),
            pltpu.VMEM((chips, HALF, toks, feat // HALF), BF16),
            pltpu.VMEM((chips, HALF, toks, feat // HALF), BF16),
            pltpu.VMEM((chips, HALF, toks, feat // HALF), BF16),
            pltpu.VMEM((n_seq, chips, tok, feat), BF16),
            dma((4,)),
            dma,
            dma,
            dma,
            dma,
            dma,
            dma,
            dma,
            dma,
            dma((n_rep, n_seq)),
            dma((chips, HALF)),
            dma((n_seq, chips)),
            dma,
        ],
        compiler_params=pltpu.CompilerParams(
            collective_id=0, has_side_effects=True, vmem_limit_bytes=62 * 1024 * 1024
        ),
    )(
        block_order,
        queries,
        keys_new,
        values_new,
        keys_past,
        values_past,
        residual,
        norm_gain.reshape(1, -1),
        router.T,
        expert_ids.T,
        out_proj,
        w_gate,
        w_up,
        w_down,
    )
    return pl.pallas_call(
        hand_over,
        out_shape=tuple(jax.ShapeDtypeStruct(out.shape, out.dtype) for out in outs),
        in_specs=[hbm] * 4,
        out_specs=(hbm,) * 4,
        scratch_shapes=[dma((4,))],
    )(*[pltpu.with_memory_space_constraint(out, pltpu.VMEM) for out in outs])


def body(*arrays):
    queries, out_proj = arrays[0], arrays[7]
    n_seq, n_rep = lax.axis_size("seq"), lax.axis_size("rep")
    held = 2 * sum(math.prod(array.shape) for array in arrays[10:13])
    tok, width, hd = queries.shape[0], queries.shape[1], arrays[1].shape[1]
    fits = held <= 50 * 1024 * 1024 and n_seq == n_rep and n_rep == 4
    fits = fits and 2 * tok * (width // hd) == hd == 128 and tok % 16 == 0
    if fits and out_proj.shape[0] == queries.shape[1]:
        return fused_body(*arrays)
    return plain_body(*arrays)


def solution(mesh):
    in_specs = (
        P(("groups", "seq"), "rep"),
        P(("groups", "seq"), "rep"),
        P(("groups", "seq"), "rep"),
        P(("groups", "seq"), "rep"),
        P(("groups", "seq"), "rep"),
        P("groups"),
        P(("groups", "seq"), "rep"),
        P("seq", "rep"),
        P(),
        P(),
        P("rep", None, "seq"),
        P("rep", None, "seq"),
        P("rep", "seq", None),
        P(("groups", "seq"), None),
    )
    out_specs = (
        P(("groups", "seq"), "rep"),
        P(("groups", "seq"), "rep"),
        P(("groups", "seq"), None),
        P(("groups", "seq"), None),
    )
    return jax.shard_map(body, mesh=mesh, in_specs=in_specs, out_specs=out_specs, check_vma=False)
```

```python
import functools
import math

import jax
import jax.numpy as jnp
from jax import lax
from jax.experimental import pallas as pl
from jax.experimental.pallas import tpu as pltpu
from jax.sharding import PartitionSpec as P

EXPERTS = 4
CAP = 12


def block_lookup(owners, block_order):
    width = block_order.shape[0]
    hits = owners[:, None] == jnp.arange(width, dtype=jnp.int32)[None, :]
    return jnp.sum(jnp.where(hits, block_order[None, :], 0), axis=1)


def plain_body(
    queries,
    keys_new,
    values_new,
    keys_past,
    values_past,
    block_order,
    residual,
    out_proj,
    norm_gain,
    router,
    w_gate,
    w_up,
    w_down,
    expert_ids,
):
    seq_index = lax.axis_index("seq")
    rep_index = lax.axis_index("rep")
    rep_count = lax.axis_size("rep")
    tok_count = queries.shape[0]
    head_dim = keys_new.shape[1]
    q_per = queries.shape[1] // head_dim
    past_len = keys_past.shape[0]
    key_span = past_len + tok_count
    row_total = tok_count * q_per
    my_block = block_lookup(jnp.full((1,), seq_index, jnp.int32), block_order)[0]
    scaling = 1.0 / math.sqrt(head_dim)
    query_rows = queries.reshape(row_total, head_dim)
    query_pos = my_block * tok_count + jnp.arange(row_total, dtype=jnp.int32) // q_per
    keys_local = jnp.concatenate([keys_past, keys_new], axis=0)
    values_local = jnp.concatenate([values_past, values_new], axis=0)
    running = jnp.full((row_total,), -1e30, jnp.float32)
    key_piece = lax.all_gather(keys_local, "seq", axis=0, tiled=True)
    value_piece = lax.all_gather(values_local, "seq", axis=0, tiled=True)
    row_count = key_piece.shape[0]
    key_index = jnp.arange(row_count, dtype=jnp.int32)
    key_owner = key_index // key_span
    offset = key_index % key_span
    key_pos = block_lookup(key_owner, block_order) * tok_count + offset - past_len
    visible = (offset < past_len)[None, :] | (key_pos[None, :] <= query_pos[:, None])
    scores = jnp.dot(query_rows, key_piece.T, preferred_element_type=jnp.float32) * scaling
    highest = jnp.maximum(running, jnp.max(jnp.where(visible, scores, -1e30), axis=1))
    weights = jnp.where(visible, jnp.exp(scores - highest[:, None]), 0.0)
    totals = jnp.sum(weights, axis=1)
    numerator = jnp.dot(
        weights.astype(jnp.bfloat16), value_piece, preferred_element_type=jnp.float32
    )
    running, totals, numerator = (highest, totals, numerator)
    attn_local = (
        (numerator / totals[:, None]).reshape(tok_count, q_per * head_dim).astype(jnp.bfloat16)
    )
    attn_full, keys_cache, values_cache = (
        lax.all_gather(attn_local, "rep", axis=1, tiled=True),
        lax.all_gather(keys_new, "rep", axis=1, tiled=True),
        lax.all_gather(values_new, "rep", axis=1, tiled=True),
    )
    head_rows = lax.all_to_all(attn_full, "seq", split_axis=1, concat_axis=0, tiled=True)
    projected = lax.psum_scatter(
        jnp.dot(head_rows, out_proj, preferred_element_type=jnp.float32).astype(jnp.bfloat16),
        "seq",
        scatter_dimension=0,
        tiled=True,
    ).astype(jnp.float32)
    attended = (residual.astype(jnp.float32) + projected).astype(jnp.bfloat16)
    full_rows = lax.all_gather(attended, "rep", axis=1, tiled=True)
    features = full_rows.astype(jnp.float32)
    mean_square = jnp.mean(features * features, axis=1, keepdims=True)
    normed = (features * norm_gain[None, :] * lax.rsqrt(mean_square + 1e-05)).astype(jnp.bfloat16)
    logits = jnp.dot(normed.astype(jnp.float32), router, precision=lax.Precision.HIGHEST)
    expert_range = jnp.arange(EXPERTS, dtype=jnp.int32)
    first_pick = (expert_ids[:, 0:1] == expert_range[None, :]).astype(jnp.float32)
    second_pick = (expert_ids[:, 1:2] == expert_range[None, :]).astype(jnp.float32)
    share_first = jax.nn.sigmoid(
        jnp.sum(first_pick * logits, axis=1) - jnp.sum(second_pick * logits, axis=1)
    )
    token_share = share_first[:, None] * first_pick + (1.0 - share_first)[:, None] * second_pick
    member = first_pick + second_pick
    ranking = jnp.cumsum(member, axis=0) - member
    slot_range = jnp.arange(CAP, dtype=jnp.float32)
    selection = member.T[:, None, :] * (ranking.T[:, None, :] == slot_range[None, :, None]).astype(
        jnp.float32
    )
    mine_mask = (expert_range == rep_index % EXPERTS).astype(jnp.float32)
    my_selection = jnp.einsum("e,ejt->jt", mine_mask, selection)
    slot_rows = jnp.dot(
        my_selection.astype(jnp.bfloat16), normed, preferred_element_type=jnp.float32
    ).astype(jnp.bfloat16)
    gate_local = w_gate[0]
    up_local = w_up[0]
    down_local = w_down[0]
    piece = lax.all_gather(slot_rows, "seq", axis=0, tiled=True)
    gate_part = jnp.dot(piece, gate_local, preferred_element_type=jnp.float32)
    up_part = jnp.dot(piece, up_local, preferred_element_type=jnp.float32)
    hidden_slots = (jax.nn.silu(gate_part) * up_part).astype(jnp.bfloat16)
    expert_part = lax.psum_scatter(
        jnp.dot(hidden_slots, down_local, preferred_element_type=jnp.float32).astype(jnp.bfloat16),
        "seq",
        scatter_dimension=0,
        tiled=True,
    ).astype(jnp.float32)
    returned = lax.all_to_all(
        expert_part.astype(jnp.bfloat16), "rep", split_axis=1, concat_axis=0, tiled=True
    ).astype(expert_part.dtype)
    source_expert = jnp.arange(rep_count, dtype=jnp.int32) % EXPERTS
    source_pick = (source_expert[:, None] == expert_range[None, :]).astype(jnp.float32)
    combine = jnp.einsum("re,ejt,te->trj", source_pick, selection, token_share).reshape(
        tok_count, rep_count * CAP
    )
    moe_slice = jnp.dot(combine, returned, precision=lax.Precision.HIGHEST)
    layer_out = (attended.astype(jnp.float32) + moe_slice).astype(jnp.bfloat16)
    return (attended, layer_out, keys_cache, values_cache)


MESH = pl.DeviceIdType.MESH
HALF = 2
F32 = jnp.float32
BF16 = jnp.bfloat16


def fused_kernel(
    n_seq,
    n_rep,
    order_hbm,
    q_hbm,
    kn_hbm,
    vn_hbm,
    kp_hbm,
    vp_hbm,
    res_hbm,
    gain_hbm,
    router_hbm,
    ids_hbm,
    proj_hbm,
    gate_hbm,
    up_hbm,
    down_hbm,
    att_out,
    layer_out,
    kc_out,
    vc_out,
    order_ref,
    q_ref,
    kn_ref,
    vn_ref,
    kp_ref,
    vp_ref,
    res_ref,
    gain_ref,
    router_ref,
    ids_ref,
    in_sem,
    wproj,
    wgate,
    wup,
    wdown,
    qall,
    idall,
    kcache,
    vcache,
    num_send,
    num_all,
    head_send,
    head_all,
    res_all,
    part_send,
    part_all,
    xall,
    gained,
    router_split,
    gate_acc,
    up_acc,
    hidden,
    ysend,
    yall,
    psend,
    fin_all,
    w_sem,
    q_rsem,
    side_rsem,
    cache_rsem,
    cache_ssem,
    num_rsem,
    head_ssem,
    head_rsem,
    part_rsem,
    x_rsem,
    y_rsem,
    z_rsem,
    send_sem,
):
    group = lax.axis_index("groups")
    seq = lax.axis_index("seq")
    rep = lax.axis_index("rep")
    tok, width = q_ref.shape
    hd = kn_ref.shape[1]
    q_per = width // hd
    toks = tok * n_seq
    feat = res_ref.shape[1]
    slab = feat // n_seq
    stat_rows = num_send.shape[1] - tok * q_per

    chips = n_rep // 2
    chip, core = rep // 2, lax.rem(rep, 2)
    partner = chip * 2 + 1 - core

    def same_core(step):
        return lax.rem(chip + step, chips) * 2 + core

    def other_core(step):
        return lax.rem(chip + step, chips) * 2 + 1 - core

    def dev(s, r):
        return {"groups": group, "seq": s, "rep": r}

    def other(index, step, size):
        return lax.rem(index + step, size)

    def remote(src, dst, ssem, rsem, s, r):
        return pltpu.make_async_remote_copy(
            src_ref=src,
            dst_ref=dst,
            send_sem=ssem,
            recv_sem=rsem,
            device_id=dev(s, r),
            device_id_type=MESH,
        )

    def rows_of(index):
        return pl.ds(pl.multiple_of(index * tok, tok), tok)

    def split_terms(rest):
        terms = []
        for _ in range(3):
            terms.append(rest.astype(BF16).astype(F32))
            rest = rest - terms[-1]
        return terms

    def size_of(ref):
        return math.prod(ref.shape) * ref.dtype.itemsize

    def wait_all(sem, size):
        tiles = size // (16 * 128 * 2)
        wide = max(w for w in range(1, wgate.shape[1] // 128 + 1) if tiles % w == 0)
        span = wgate.at[pl.ds(0, tiles // wide * 16), pl.ds(0, wide * 128)]
        pltpu.make_async_copy(span, span, sem).wait()

    def slab_of(index):
        return pl.ds(pl.multiple_of(index * slab, slab), slab)

    def per_seq(rows):
        return [sum(jnp.where(seq == s, rows[s][k], 0) for s in range(n_seq)) for k in range(n_seq - 1)]

    def others(s):
        return [t for t in range(n_seq) if t != s]

    far_first = per_seq([sorted(others(s), key=lambda t: -abs(t - s)) for s in range(n_seq)])
    arrivals = per_seq(
        [
            sorted(others(s), key=lambda f: (abs(f - s), f if 2 * s < n_seq else -f))
            for s in range(n_seq)
        ]
    )

    smalls = [
        pltpu.make_async_copy(src, dst, in_sem.at[(0, 1, 2, 2, 3, 3, 4, 5, 6, 7)[i]])
        for i, (src, dst) in enumerate(
            (
                (ids_hbm, ids_ref),
                (q_hbm, q_ref),
                (kn_hbm, kn_ref),
                (vn_hbm, vn_ref),
                (kp_hbm, kp_ref),
                (vp_hbm, vp_ref),
                (order_hbm, order_ref),
                (res_hbm, res_ref),
                (gain_hbm, gain_ref),
                (router_hbm, router_ref),
            )
        )
    ]
    for small in smalls:
        small.start()

    barrier = pltpu.get_barrier_semaphore()
    for i in reversed(range(n_seq)):
        for j in reversed(range(n_rep)):
            if i or j:
                pl.semaphore_signal(
                    barrier,
                    inc=1,
                    device_id=dev(other(seq, i, n_seq), other(rep, j, n_rep)),
                    device_id_type=MESH,
                )

    loads = []
    for i, (src, dst) in enumerate(
        ((proj_hbm, wproj), (gate_hbm.at[0], wgate), (up_hbm.at[0], wup), (down_hbm.at[0], wdown))
    ):
        pieces = 1 if i == 0 else 4
        size = dst.shape[0] // pieces
        for j in range(pieces):
            span = pl.ds(j * size, size)
            pltpu.make_async_copy(src.at[span], dst.at[span], w_sem.at[i]).start()
        loads.append(pltpu.make_async_copy(src, dst, w_sem.at[i]))

    smalls[0].wait()
    smalls[1].wait()
    wait_all(in_sem.at[2], 2 * size_of(kn_ref))
    lane = lax.broadcasted_iota(jnp.int32, (tok, 128), 1)
    ids_f = ids_ref[...].astype(F32)
    diagonal = lax.broadcasted_iota(jnp.int32, (tok, tok), 0) == lax.broadcasted_iota(
        jnp.int32, (tok, tok), 1
    )
    picks = [
        jnp.sum(jnp.where(diagonal, ids_f[i : i + 1, :], 0.0), axis=1, keepdims=True)
        for i in range(2)
    ]
    idall[rows_of(seq), :] = jnp.where(lane == 0, picks[0], picks[1])
    qall[rows_of(seq), :] = q_ref[...]
    for j in range(n_rep):

        @pl.when(rep == j)
        def _():
            kcache[:, j * hd : (j + 1) * hd] = kn_ref[...]
            vcache[:, j * hd : (j + 1) * hd] = vn_ref[...]

    pl.semaphore_wait(barrier, n_seq * n_rep - 1)

    sent = [0]

    def send(ref, *rest):
        sent[0] += size_of(ref)
        remote(ref, rest[0], send_sem, *rest[1:]).start()

    mine = rows_of(seq)
    for to in far_first:
        send(q_ref, qall.at[mine], q_rsem.at[seq], to, rep)

    experts = router_ref.shape[0]
    wait_all(in_sem.at[3], 2 * size_of(kp_ref))
    for small in smalls[6:]:
        small.wait()
    own_pos = order_ref[seq] * tok + lax.broadcasted_iota(jnp.int32, (tok, tok), 1)
    terms = split_terms(router_ref[...])
    terms.append(jnp.zeros((router_split.shape[0] - 3 * experts, router_ref.shape[1]), F32))
    router_split[...] = jnp.concatenate(terms, axis=0).astype(BF16)
    for to in far_first:
        send(res_ref.at[:, slab_of(to)], res_all.at[mine], side_rsem, to, rep)
        send(idall.at[mine], idall.at[mine], side_rsem, to, rep)
    res_all[mine, :] = res_ref[:, slab_of(seq)]
    for j in range(n_rep):

        @pl.when(rep == j)
        def _():
            cols = pl.ds(j * hd, hd)
            for k in range(1, n_rep):
                to = (j + k) % n_rep
                remote(kn_ref, kcache.at[:, cols], cache_ssem, cache_rsem, seq, to).start()
                remote(vn_ref, vcache.at[:, cols], cache_ssem, cache_rsem, seq, to).start()

    scaling = 1.0 / math.sqrt(hd)
    nt = (((1,), (1,)), ((), ()))
    span = tok * q_per
    row = lax.broadcasted_iota(jnp.int32, (tok, tok), 0)

    def attend(t, out):
        block = qall[rows_of(t), :]
        block = jnp.concatenate([block[:, h * hd : (h + 1) * hd] for h in range(q_per)], axis=0)
        bias = jnp.where(own_pos <= order_ref[t] * tok + row, 0.0, -1e30)
        bias = jnp.concatenate([bias] * q_per, axis=0)
        s_past = lax.dot_general(block, kp_ref[...], nt, preferred_element_type=F32) * scaling
        s_new = lax.dot_general(block, kn_ref[...], nt, preferred_element_type=F32) * scaling + bias
        high = jnp.maximum(
            jnp.max(s_past, axis=1, keepdims=True), jnp.max(s_new, axis=1, keepdims=True)
        )
        w_past = jnp.exp(s_past - high)
        w_new = jnp.exp(s_new - high)
        total = jnp.sum(w_past, axis=1, keepdims=True) + jnp.sum(w_new, axis=1, keepdims=True)
        num = jnp.dot(w_past.astype(BF16), vp_ref[...], preferred_element_type=F32) + jnp.dot(
            w_new.astype(BF16), vn_ref[...], preferred_element_type=F32
        )
        stat_lane = lax.broadcasted_iota(jnp.int32, (span, 128), 1)
        stats = jnp.where(stat_lane == 0, high, total).T
        line = jnp.concatenate([stats[i : i + 1, :] for i in range(2)], axis=1)
        coded = split_terms(line) + [jnp.zeros((stat_rows - 3, 2 * span), F32)]
        out[:span, :] = num.astype(BF16)
        out[span:, :] = jnp.concatenate(coded, axis=0).astype(BF16)

    attend(seq, num_all.at[seq])
    for frm in arrivals:
        src = rows_of(frm)
        remote(q_ref, qall.at[src], send_sem, q_rsem.at[frm], frm, rep).wait_recv()
        attend(frm, num_send.at[frm])
        send(num_send.at[frm], num_all.at[seq], num_rsem, frm, rep)

    wait_all(num_rsem, (n_seq - 1) * size_of(num_send.at[0]))

    lines = []
    for i in range(n_seq):
        coded = num_all[i, span:, :].astype(F32)
        lines.append(coded[0:1] + coded[1:2] + coded[2:3])
    lines.append(jnp.zeros((128 - n_seq, 2 * span), F32))
    stat_cols = jnp.concatenate(lines, axis=0).T
    highs = [stat_cols[:span, i : i + 1] for i in range(n_seq)]
    top = functools.reduce(jnp.maximum, highs)
    scales = [jnp.exp(h - top) for h in highs]
    full = sum(scales[i] * stat_cols[span:, i : i + 1] for i in range(n_seq))
    heads = sum(scales[i] * num_all[i, :span, :].astype(F32) for i in range(n_seq)) / full
    head_send[...] = heads.astype(BF16)

    def head_copy(to):
        return remote(head_send, head_all.at[seq], head_ssem, head_rsem.at[seq], rep, to)

    for j in range(1, chips):
        send(head_send, head_all.at[seq], head_rsem.at[seq], rep, same_core(j))
        send(head_send, head_all.at[seq], head_rsem.at[seq], rep, other_core(j))

    @pl.when(seq != rep)
    def _():
        head_copy(rep).start()

    send(head_send, head_all.at[seq], head_rsem.at[seq], rep, partner)
    loads[0].wait()

    def head_wait(f):
        remote(head_send, head_all.at[f], head_ssem, head_rsem.at[f], seq, rep).wait_recv()

    def project(f):
        block = jnp.concatenate(
            [head_all[f, h * tok : (h + 1) * tok, :] for h in range(q_per)], axis=1
        )
        part = jnp.dot(block, wproj[...], preferred_element_type=F32).astype(BF16)
        for t in range(n_seq):
            part_send[f, t] = part[:, t * slab : (t + 1) * slab]
        for to in far_first:
            send(part_send.at[f, to], part_all.at[seq, rows_of(f)], part_rsem, to, rep)
        part_all[seq, rows_of(f), :] = part_send[f, seq]

    @pl.when(seq == rep)
    def _():
        head_all[seq] = head_send[...]

    @pl.when(seq != rep)
    def _():
        head_wait(seq)

    project(seq)
    for f in arrivals:
        head_wait(f)
        project(f)

    wait_all(side_rsem, (n_seq - 1) * (tok * slab * 2 + tok * 128 * 4))

    @pl.when(seq != rep)
    def _():
        head_copy(rep).wait_send()

    wait_all(part_rsem, (n_seq - 1) * toks * slab * 2)
    summed = sum(part_all[f].astype(F32) for f in range(n_seq))
    xall[rep, seq] = (res_all[...].astype(F32) + summed).astype(BF16)

    def x_send(r, s, to_s, to_r):
        view = xall.at[r, s]
        send(view, view, x_rsem.at[r, s], to_s, to_r)

    def arrive(r, s):
        view = xall.at[r, s]
        remote(view, view, send_sem, x_rsem.at[r, s], seq, r).wait_recv()

    def spread(s, direct):
        for j in range(1, chips):
            x_send(rep, s, seq, same_core(j))
            if direct:
                x_send(rep, s, seq, other_core(j))
        x_send(rep, s, seq, partner)

    def from_seq(k):
        arrive(rep, arrivals[k])
        spread(arrivals[k], k > 0)

    def from_chip(s):
        for j in range(1, chips):
            arrive(same_core(j), s)
            x_send(same_core(j), s, seq, partner)

    spread(seq, False)
    for to in reversed(far_first):
        x_send(rep, seq, to, rep)
    hidden_width = wgate.shape[1]
    chunk = min(512, hidden_width)
    squares = [jnp.zeros((toks, 128), F32)]
    logits = [jnp.zeros((toks, router_split.shape[0]), F32)]

    def prepare(slots):
        for i, (r, s) in enumerate(slots):
            cols = pl.ds(pl.multiple_of(r * feat + s * slab, slab), slab)
            part = xall[r, s].astype(F32)
            squared = part * part
            for j in range(slab // 128):
                squares[0] = squares[0] + squared[:, j * 128 : (j + 1) * 128]
            scaled = (part * gain_ref[:, cols]).astype(BF16)
            gained[:, i * slab : (i + 1) * slab] = scaled
            logits[0] = logits[0] + lax.dot_general(
                scaled, router_split[:, cols], nt, preferred_element_type=F32
            )

    def products(slots, cols):
        total = None
        for i, (r, s) in enumerate(slots):
            span = pl.ds(pl.multiple_of(r * feat + s * slab, slab), slab)
            block = gained[:, i * slab : (i + 1) * slab]
            pair = (
                jnp.dot(block, wgate[span, cols], preferred_element_type=F32),
                jnp.dot(block, wup[span, cols], preferred_element_type=F32),
            )
            total = pair if total is None else (total[0] + pair[0], total[1] + pair[1])
        return total

    def add_slots(slots, start=False):
        prepare(slots)
        for c in range(hidden_width // chunk):
            cols = pl.ds(c * chunk, chunk)
            gate, up = products(slots, cols)
            if start:
                gate_acc[:, cols] = gate
                up_acc[:, cols] = up
            else:
                gate_acc[:, cols] += gate
                up_acc[:, cols] += up

    for load in loads[1:3]:
        load.wait()
    arrive(partner, seq)
    add_slots([(rep, seq), (partner, seq)], True)
    from_seq(0)
    from_chip(seq)
    from_seq(1)
    add_slots([(rep, arrivals[0]), (same_core(1), seq)])
    for k in range(2, n_seq - 1):
        from_seq(k)
    att_out[...] = jnp.concatenate([xall[rep, t, mine] for t in range(n_seq)], axis=1)
    arrive(partner, arrivals[0])
    arrive(other_core(1), seq)
    add_slots([(partner, arrivals[0]), (other_core(1), seq)])
    rest = arrivals[1:]
    add_slots([(rep, s) for s in rest])
    from_chip(arrivals[0])
    for s in rest:
        arrive(partner, s)
    add_slots([(partner, s) for s in rest])
    for s in rest[:-1]:
        arrive(same_core(1), s)
    add_slots([(same_core(1), s) for s in arrivals[:-1]])
    for s in arrivals[:-1]:
        arrive(other_core(1), s)
    add_slots([(other_core(1), s) for s in arrivals[:-1]])
    loads[3].wait()
    final = [(same_core(1), arrivals[-1]), (other_core(1), arrivals[-1])]
    for slot in final:
        arrive(*slot)
    prepare(final)
    square = jnp.sum(squares[0], axis=1, keepdims=True)
    inverse = lax.rsqrt(square / (feat * n_rep) + 1e-05)
    for c in range(hidden_width // chunk):
        cols = pl.ds(c * chunk, chunk)
        gate, up = products(final, cols)
        gate = (gate_acc[:, cols] + gate) * inverse
        up = (up_acc[:, cols] + up) * inverse
        hidden[:, cols] = (gate * jax.nn.sigmoid(gate) * up).astype(BF16)

    columns = [
        sum(logits[0][:, i * experts + e : i * experts + e + 1] for i in range(3)) * inverse
        for e in range(experts)
    ]
    first = [(idall[:, 0:1] == float(e)).astype(F32) for e in range(experts)]
    second = [(idall[:, 1:2] == float(e)).astype(F32) for e in range(experts)]
    gap = sum(first[e] * columns[e] for e in range(experts)) - sum(
        second[e] * columns[e] for e in range(experts)
    )
    share = jax.nn.sigmoid(gap)
    mine_first = (idall[:, 0:1] == (rep % experts).astype(F32)).astype(F32)
    mine_second = (idall[:, 1:2] == (rep % experts).astype(F32)).astype(F32)
    weight = share * mine_first + (1.0 - share) * mine_second

    def weighted(to_chip, to_core, at, size):
        start = (to_chip * 2 + to_core) * feat + at
        cols = pl.ds(pl.multiple_of(start, size), size)
        return jnp.dot(hidden[...], wdown[:, cols], preferred_element_type=F32) * weight

    def cross(j, h, parts):
        size = feat // parts
        cols = pl.ds(h * size, size)
        ysend[j, :, cols] = weighted(lax.rem(chip + j, chips), 1 - core, h * size, size).astype(BF16)
        send(ysend.at[j, :, cols], yall.at[j, :, cols], y_rsem.at[j, h], seq, partner)

    def keep(j, h, parts):
        size = feat // parts
        cols = pl.ds(h * size, size)
        product = weighted(lax.rem(chip + j, chips), core, h * size, size)
        view = yall.at[j, :, cols]
        remote(view, view, send_sem, y_rsem.at[j, h], seq, partner).wait_recv()
        psend[j, :, cols] = (product + yall[j, :, cols].astype(F32)).astype(BF16)
        owner = lax.rem(chip + j, chips) * 2 + core
        for to in far_first + [seq] * min(j, 1):
            place = fin_all.at[seq, chip, :, cols]
            send(psend.at[j, rows_of(to), cols], place, z_rsem.at[seq, chip], to, owner)

    for j in range(1, chips):
        for h in range(HALF):
            cross(j, h, HALF)
    for j in range(1, chips):
        for h in range(HALF):
            keep(j, h, HALF)
    cross(0, 0, 1)
    keep(0, 0, 1)

    wait_all(cache_rsem, 2 * (n_rep - 1) * size_of(kn_ref))
    kc_out[...] = kcache[...]
    vc_out[...] = vcache[...]
    wait_all(cache_ssem, 2 * (n_rep - 1) * size_of(kn_ref))
    wait_all(send_sem, sent[0])

    result = att_out[...].astype(F32) + psend[0, mine, :].astype(F32)
    for frm_s, frm_chip in [(seq, lax.rem(chip + j, chips)) for j in range(1, chips)] + [
        (s, lax.rem(chip + j, chips)) for s in arrivals for j in range(chips)
    ]:
        place = fin_all.at[frm_s, frm_chip]
        remote(place, place, send_sem, z_rsem.at[frm_s, frm_chip], frm_s, rep).wait_recv()
        result = result + fin_all[frm_s, frm_chip].astype(F32)
    layer_out[...] = result.astype(BF16)


def hand_over(*refs):
    sem = refs[8]
    copies = [pltpu.make_async_copy(refs[i], refs[4 + i], sem.at[i]) for i in range(4)]
    for copy in copies:
        copy.start()
    for copy in copies:
        copy.wait()


def fused_body(
    queries,
    keys_new,
    values_new,
    keys_past,
    values_past,
    block_order,
    residual,
    out_proj,
    norm_gain,
    router,
    w_gate,
    w_up,
    w_down,
    expert_ids,
):
    n_seq = lax.axis_size("seq")
    n_rep = lax.axis_size("rep")
    tok, width = queries.shape
    hd = keys_new.shape[1]
    toks = tok * n_seq
    rows = toks * (width // hd)
    feat = residual.shape[1]
    slab = feat // n_seq
    chips = n_rep // 2
    vmem = pl.BlockSpec(memory_space=pltpu.VMEM)
    hbm = pl.BlockSpec(memory_space=pl.ANY)
    dma = pltpu.SemaphoreType.DMA
    cache = (tok, hd * n_rep)
    outs = pl.pallas_call(
        functools.partial(fused_kernel, n_seq, n_rep),
        out_shape=(
            pltpu.VMEM((tok, feat), BF16),
            pltpu.VMEM((tok, feat), BF16),
            pltpu.VMEM(cache, BF16),
            pltpu.VMEM(cache, BF16),
        ),
        in_specs=[hbm] * 14,
        out_specs=(vmem,) * 4,
        scratch_shapes=[
            pltpu.SMEM(block_order.shape, jnp.int32),
            pltpu.VMEM(queries.shape, BF16),
            pltpu.VMEM(keys_new.shape, BF16),
            pltpu.VMEM(values_new.shape, BF16),
            pltpu.VMEM(keys_past.shape, BF16),
            pltpu.VMEM(values_past.shape, BF16),
            pltpu.VMEM(residual.shape, BF16),
            pltpu.VMEM((1, norm_gain.shape[0]), F32),
            pltpu.VMEM(router.shape[::-1], F32),
            pltpu.VMEM(expert_ids.shape[::-1], jnp.int32),
            dma((9,)),
            pltpu.VMEM(out_proj.shape, BF16),
            pltpu.VMEM(w_gate.shape[1:], BF16),
            pltpu.VMEM(w_up.shape[1:], BF16),
            pltpu.VMEM(w_down.shape[1:], BF16),
            pltpu.VMEM((toks, width), BF16),
            pltpu.VMEM((toks, 128), F32),
            pltpu.VMEM(cache, BF16),
            pltpu.VMEM(cache, BF16),
            pltpu.VMEM((n_seq, rows // n_seq + 16, hd), BF16),
            pltpu.VMEM((n_seq, rows // n_seq + 16, hd), BF16),
            pltpu.VMEM((rows // n_seq, hd), BF16),
            pltpu.VMEM((n_seq, rows // n_seq, hd), BF16),
            pltpu.VMEM((toks, slab), BF16),
            pltpu.VMEM((n_seq, n_seq, tok, slab), BF16),
            pltpu.VMEM((n_seq, toks, slab), BF16),
            pltpu.VMEM((n_rep, n_seq, toks, slab), BF16),
            pltpu.VMEM((toks, (n_seq - 2) * slab), BF16),
            pltpu.VMEM((16, norm_gain.shape[0]), BF16),
            pltpu.VMEM((toks, w_gate.shape[2]), F32),
            pltpu.VMEM((toks, w_gate.shape[2]), F32),
            pltpu.VMEM((toks, w_gate.shape[2]), BF16),
            pltpu.VMEM((chips, toks, feat), BF16),
            pltpu.VMEM((chips, toks, feat), BF16),
            pltpu.VMEM((chips, toks, feat), BF16),
            pltpu.VMEM((n_seq, chips, tok, feat), BF16),
            dma((4,)),
            dma((n_seq,)),
            dma,
            dma,
            dma,
            dma,
            dma,
            dma((n_seq,)),
            dma,
            dma((n_rep, n_seq)),
            dma((chips, HALF)),
            dma((n_seq, chips)),
            dma,
        ],
        compiler_params=pltpu.CompilerParams(
            collective_id=0, has_side_effects=True, vmem_limit_bytes=62 * 1024 * 1024
        ),
    )(
        block_order,
        queries,
        keys_new,
        values_new,
        keys_past,
        values_past,
        residual,
        norm_gain.reshape(1, -1),
        router.T,
        expert_ids.T,
        out_proj,
        w_gate,
        w_up,
        w_down,
    )
    return pl.pallas_call(
        hand_over,
        out_shape=tuple(jax.ShapeDtypeStruct(out.shape, out.dtype) for out in outs),
        in_specs=[hbm] * 4,
        out_specs=(hbm,) * 4,
        scratch_shapes=[dma((4,))],
    )(*[pltpu.with_memory_space_constraint(out, pltpu.VMEM) for out in outs])


def body(*arrays):
    queries, out_proj = arrays[0], arrays[7]
    n_seq, n_rep = lax.axis_size("seq"), lax.axis_size("rep")
    held = 2 * sum(math.prod(array.shape) for array in arrays[10:13])
    tok, width, hd = queries.shape[0], queries.shape[1], arrays[1].shape[1]
    fits = held <= 50 * 1024 * 1024 and n_seq == n_rep and n_rep == 4
    fits = fits and 2 * tok * (width // hd) == hd == 128 and tok % 16 == 0
    if fits and out_proj.shape[0] == queries.shape[1]:
        return fused_body(*arrays)
    return plain_body(*arrays)


def solution(mesh):
    in_specs = (
        P(("groups", "seq"), "rep"),
        P(("groups", "seq"), "rep"),
        P(("groups", "seq"), "rep"),
        P(("groups", "seq"), "rep"),
        P(("groups", "seq"), "rep"),
        P("groups"),
        P(("groups", "seq"), "rep"),
        P("seq", "rep"),
        P(),
        P(),
        P("rep", None, "seq"),
        P("rep", None, "seq"),
        P("rep", "seq", None),
        P(("groups", "seq"), None),
    )
    out_specs = (
        P(("groups", "seq"), "rep"),
        P(("groups", "seq"), "rep"),
        P(("groups", "seq"), None),
        P(("groups", "seq"), None),
    )
    return jax.shard_map(body, mesh=mesh, in_specs=in_specs, out_specs=out_specs, check_vma=False)
```

```python
import functools
import math

import jax
import jax.numpy as jnp
from jax import lax
from jax.experimental import pallas as pl
from jax.experimental.pallas import tpu as pltpu
from jax.sharding import PartitionSpec as P

EXPERTS = 4
CAP = 12


def block_lookup(owners, block_order):
    width = block_order.shape[0]
    hits = owners[:, None] == jnp.arange(width, dtype=jnp.int32)[None, :]
    return jnp.sum(jnp.where(hits, block_order[None, :], 0), axis=1)


def plain_body(
    queries,
    keys_new,
    values_new,
    keys_past,
    values_past,
    block_order,
    residual,
    out_proj,
    norm_gain,
    router,
    w_gate,
    w_up,
    w_down,
    expert_ids,
):
    seq_index = lax.axis_index("seq")
    rep_index = lax.axis_index("rep")
    rep_count = lax.axis_size("rep")
    tok_count = queries.shape[0]
    head_dim = keys_new.shape[1]
    q_per = queries.shape[1] // head_dim
    past_len = keys_past.shape[0]
    key_span = past_len + tok_count
    row_total = tok_count * q_per
    my_block = block_lookup(jnp.full((1,), seq_index, jnp.int32), block_order)[0]
    scaling = 1.0 / math.sqrt(head_dim)
    query_rows = queries.reshape(row_total, head_dim)
    query_pos = my_block * tok_count + jnp.arange(row_total, dtype=jnp.int32) // q_per
    keys_local = jnp.concatenate([keys_past, keys_new], axis=0)
    values_local = jnp.concatenate([values_past, values_new], axis=0)
    running = jnp.full((row_total,), -1e30, jnp.float32)
    key_piece = lax.all_gather(keys_local, "seq", axis=0, tiled=True)
    value_piece = lax.all_gather(values_local, "seq", axis=0, tiled=True)
    row_count = key_piece.shape[0]
    key_index = jnp.arange(row_count, dtype=jnp.int32)
    key_owner = key_index // key_span
    offset = key_index % key_span
    key_pos = block_lookup(key_owner, block_order) * tok_count + offset - past_len
    visible = (offset < past_len)[None, :] | (key_pos[None, :] <= query_pos[:, None])
    scores = jnp.dot(query_rows, key_piece.T, preferred_element_type=jnp.float32) * scaling
    highest = jnp.maximum(running, jnp.max(jnp.where(visible, scores, -1e30), axis=1))
    weights = jnp.where(visible, jnp.exp(scores - highest[:, None]), 0.0)
    totals = jnp.sum(weights, axis=1)
    numerator = jnp.dot(
        weights.astype(jnp.bfloat16), value_piece, preferred_element_type=jnp.float32
    )
    running, totals, numerator = (highest, totals, numerator)
    attn_local = (
        (numerator / totals[:, None]).reshape(tok_count, q_per * head_dim).astype(jnp.bfloat16)
    )
    attn_full, keys_cache, values_cache = (
        lax.all_gather(attn_local, "rep", axis=1, tiled=True),
        lax.all_gather(keys_new, "rep", axis=1, tiled=True),
        lax.all_gather(values_new, "rep", axis=1, tiled=True),
    )
    head_rows = lax.all_to_all(attn_full, "seq", split_axis=1, concat_axis=0, tiled=True)
    projected = lax.psum_scatter(
        jnp.dot(head_rows, out_proj, preferred_element_type=jnp.float32).astype(jnp.bfloat16),
        "seq",
        scatter_dimension=0,
        tiled=True,
    ).astype(jnp.float32)
    attended = (residual.astype(jnp.float32) + projected).astype(jnp.bfloat16)
    full_rows = lax.all_gather(attended, "rep", axis=1, tiled=True)
    features = full_rows.astype(jnp.float32)
    mean_square = jnp.mean(features * features, axis=1, keepdims=True)
    normed = (features * norm_gain[None, :] * lax.rsqrt(mean_square + 1e-05)).astype(jnp.bfloat16)
    logits = jnp.dot(normed.astype(jnp.float32), router, precision=lax.Precision.HIGHEST)
    expert_range = jnp.arange(EXPERTS, dtype=jnp.int32)
    first_pick = (expert_ids[:, 0:1] == expert_range[None, :]).astype(jnp.float32)
    second_pick = (expert_ids[:, 1:2] == expert_range[None, :]).astype(jnp.float32)
    share_first = jax.nn.sigmoid(
        jnp.sum(first_pick * logits, axis=1) - jnp.sum(second_pick * logits, axis=1)
    )
    token_share = share_first[:, None] * first_pick + (1.0 - share_first)[:, None] * second_pick
    member = first_pick + second_pick
    ranking = jnp.cumsum(member, axis=0) - member
    slot_range = jnp.arange(CAP, dtype=jnp.float32)
    selection = member.T[:, None, :] * (ranking.T[:, None, :] == slot_range[None, :, None]).astype(
        jnp.float32
    )
    mine_mask = (expert_range == rep_index % EXPERTS).astype(jnp.float32)
    my_selection = jnp.einsum("e,ejt->jt", mine_mask, selection)
    slot_rows = jnp.dot(
        my_selection.astype(jnp.bfloat16), normed, preferred_element_type=jnp.float32
    ).astype(jnp.bfloat16)
    gate_local = w_gate[0]
    up_local = w_up[0]
    down_local = w_down[0]
    piece = lax.all_gather(slot_rows, "seq", axis=0, tiled=True)
    gate_part = jnp.dot(piece, gate_local, preferred_element_type=jnp.float32)
    up_part = jnp.dot(piece, up_local, preferred_element_type=jnp.float32)
    hidden_slots = (jax.nn.silu(gate_part) * up_part).astype(jnp.bfloat16)
    expert_part = lax.psum_scatter(
        jnp.dot(hidden_slots, down_local, preferred_element_type=jnp.float32).astype(jnp.bfloat16),
        "seq",
        scatter_dimension=0,
        tiled=True,
    ).astype(jnp.float32)
    returned = lax.all_to_all(
        expert_part.astype(jnp.bfloat16), "rep", split_axis=1, concat_axis=0, tiled=True
    ).astype(expert_part.dtype)
    source_expert = jnp.arange(rep_count, dtype=jnp.int32) % EXPERTS
    source_pick = (source_expert[:, None] == expert_range[None, :]).astype(jnp.float32)
    combine = jnp.einsum("re,ejt,te->trj", source_pick, selection, token_share).reshape(
        tok_count, rep_count * CAP
    )
    moe_slice = jnp.dot(combine, returned, precision=lax.Precision.HIGHEST)
    layer_out = (attended.astype(jnp.float32) + moe_slice).astype(jnp.bfloat16)
    return (attended, layer_out, keys_cache, values_cache)


MESH = pl.DeviceIdType.MESH
HALF = 2
F32 = jnp.float32
BF16 = jnp.bfloat16


def fused_kernel(
    n_seq,
    n_rep,
    order_hbm,
    q_hbm,
    kn_hbm,
    vn_hbm,
    kp_hbm,
    vp_hbm,
    res_hbm,
    gain_hbm,
    router_hbm,
    ids_hbm,
    proj_hbm,
    gate_hbm,
    up_hbm,
    down_hbm,
    att_out,
    layer_out,
    kc_out,
    vc_out,
    order_ref,
    q_ref,
    kn_ref,
    vn_ref,
    kp_ref,
    vp_ref,
    res_ref,
    gain_ref,
    router_ref,
    ids_ref,
    in_sem,
    wproj,
    wgate,
    wup,
    wdown,
    qall,
    idall,
    kcache,
    vcache,
    num_send,
    num_all,
    head_send,
    head_all,
    res_all,
    part_send,
    part_all,
    xall,
    gained,
    router_split,
    gate_acc,
    up_acc,
    hidden,
    ysend,
    yall,
    psend,
    fin_all,
    w_sem,
    q_rsem,
    side_rsem,
    cache_rsem,
    cache_ssem,
    num_rsem,
    head_ssem,
    head_rsem,
    part_rsem,
    x_rsem,
    y_rsem,
    z_rsem,
    send_sem,
):
    group = lax.axis_index("groups")
    seq = lax.axis_index("seq")
    rep = lax.axis_index("rep")
    tok, width = q_ref.shape
    hd = kn_ref.shape[1]
    q_per = width // hd
    toks = tok * n_seq
    feat = res_ref.shape[1]
    slab = feat // n_seq
    stat_rows = num_send.shape[1] - tok * q_per

    chips = n_rep // 2
    chip, core = rep // 2, lax.rem(rep, 2)
    partner = chip * 2 + 1 - core

    def same_core(step):
        return lax.rem(chip + step, chips) * 2 + core

    def other_core(step):
        return lax.rem(chip + step, chips) * 2 + 1 - core

    def dev(s, r):
        return {"groups": group, "seq": s, "rep": r}

    def other(index, step, size):
        return lax.rem(index + step, size)

    def remote(src, dst, ssem, rsem, s, r):
        return pltpu.make_async_remote_copy(
            src_ref=src,
            dst_ref=dst,
            send_sem=ssem,
            recv_sem=rsem,
            device_id=dev(s, r),
            device_id_type=MESH,
        )

    def rows_of(index):
        return pl.ds(pl.multiple_of(index * tok, tok), tok)

    def split_terms(rest):
        terms = []
        for _ in range(3):
            terms.append(rest.astype(BF16).astype(F32))
            rest = rest - terms[-1]
        return terms

    def size_of(ref):
        return math.prod(ref.shape) * ref.dtype.itemsize

    def wait_all(sem, size):
        tiles = size // (16 * 128 * 2)
        wide = max(w for w in range(1, wgate.shape[1] // 128 + 1) if tiles % w == 0)
        span = wgate.at[pl.ds(0, tiles // wide * 16), pl.ds(0, wide * 128)]
        pltpu.make_async_copy(span, span, sem).wait()

    def slab_of(index):
        return pl.ds(pl.multiple_of(index * slab, slab), slab)

    def per_seq(rows):
        return [sum(jnp.where(seq == s, rows[s][k], 0) for s in range(n_seq)) for k in range(n_seq - 1)]

    def others(s):
        return [t for t in range(n_seq) if t != s]

    far_first = per_seq([sorted(others(s), key=lambda t: -abs(t - s)) for s in range(n_seq)])
    arrivals = per_seq(
        [
            sorted(others(s), key=lambda f: (abs(f - s), f if 2 * s < n_seq else -f))
            for s in range(n_seq)
        ]
    )

    smalls = [
        pltpu.make_async_copy(src, dst, in_sem.at[(0, 1, 2, 2, 3, 3, 4, 5, 6, 7)[i]])
        for i, (src, dst) in enumerate(
            (
                (ids_hbm, ids_ref),
                (q_hbm, q_ref),
                (kn_hbm, kn_ref),
                (vn_hbm, vn_ref),
                (kp_hbm, kp_ref),
                (vp_hbm, vp_ref),
                (order_hbm, order_ref),
                (res_hbm, res_ref),
                (gain_hbm, gain_ref),
                (router_hbm, router_ref),
            )
        )
    ]
    for small in smalls:
        small.start()

    barrier = pltpu.get_barrier_semaphore()
    for i in reversed(range(n_seq)):
        for j in reversed(range(n_rep)):
            if i or j:
                pl.semaphore_signal(
                    barrier,
                    inc=1,
                    device_id=dev(other(seq, i, n_seq), other(rep, j, n_rep)),
                    device_id_type=MESH,
                )

    loads = []
    for i, (src, dst) in enumerate(
        ((proj_hbm, wproj), (gate_hbm.at[0], wgate), (up_hbm.at[0], wup), (down_hbm.at[0], wdown))
    ):
        pieces = 1 if i == 0 else 4
        size = dst.shape[0] // pieces
        for j in range(pieces):
            span = pl.ds(j * size, size)
            pltpu.make_async_copy(src.at[span], dst.at[span], w_sem.at[i]).start()
        loads.append(pltpu.make_async_copy(src, dst, w_sem.at[i]))

    smalls[0].wait()
    smalls[1].wait()
    wait_all(in_sem.at[2], 2 * size_of(kn_ref))
    lane = lax.broadcasted_iota(jnp.int32, (tok, 128), 1)
    ids_f = ids_ref[...].astype(F32)
    diagonal = lax.broadcasted_iota(jnp.int32, (tok, tok), 0) == lax.broadcasted_iota(
        jnp.int32, (tok, tok), 1
    )
    picks = [
        jnp.sum(jnp.where(diagonal, ids_f[i : i + 1, :], 0.0), axis=1, keepdims=True)
        for i in range(2)
    ]
    idall[rows_of(seq), :] = jnp.where(lane == 0, picks[0], picks[1])
    qall[rows_of(seq), :] = q_ref[...]
    for j in range(n_rep):

        @pl.when(rep == j)
        def _():
            kcache[:, j * hd : (j + 1) * hd] = kn_ref[...]
            vcache[:, j * hd : (j + 1) * hd] = vn_ref[...]

    pl.semaphore_wait(barrier, n_seq * n_rep - 1)

    sent = [0]

    def send(ref, *rest):
        sent[0] += size_of(ref)
        remote(ref, rest[0], send_sem, *rest[1:]).start()

    mine = rows_of(seq)
    for to in far_first:
        send(q_ref, qall.at[mine], q_rsem.at[seq], to, rep)

    experts = router_ref.shape[0]
    wait_all(in_sem.at[3], 2 * size_of(kp_ref))
    for small in smalls[6:]:
        small.wait()
    own_pos = order_ref[seq] * tok + lax.broadcasted_iota(jnp.int32, (tok, tok), 1)
    terms = split_terms(router_ref[...])
    terms.append(jnp.zeros((router_split.shape[0] - 3 * experts, router_ref.shape[1]), F32))
    router_split[...] = jnp.concatenate(terms, axis=0).astype(BF16)
    for to in far_first:
        send(res_ref.at[:, slab_of(to)], res_all.at[mine], side_rsem, to, rep)
        send(idall.at[mine], idall.at[mine], side_rsem, to, rep)
    res_all[mine, :] = res_ref[:, slab_of(seq)]
    for j in range(n_rep):

        @pl.when(rep == j)
        def _():
            cols = pl.ds(j * hd, hd)
            for k in range(1, n_rep):
                to = (j + k) % n_rep
                remote(kn_ref, kcache.at[:, cols], cache_ssem, cache_rsem, seq, to).start()
                remote(vn_ref, vcache.at[:, cols], cache_ssem, cache_rsem, seq, to).start()

    scaling = 1.0 / math.sqrt(hd)
    nt = (((1,), (1,)), ((), ()))
    span = tok * q_per
    row = lax.broadcasted_iota(jnp.int32, (tok, tok), 0)

    def attend(t, out):
        block = qall[rows_of(t), :]
        block = jnp.concatenate([block[:, h * hd : (h + 1) * hd] for h in range(q_per)], axis=0)
        bias = jnp.where(own_pos <= order_ref[t] * tok + row, 0.0, -1e30)
        bias = jnp.concatenate([bias] * q_per, axis=0)
        s_past = lax.dot_general(block, kp_ref[...], nt, preferred_element_type=F32) * scaling
        s_new = lax.dot_general(block, kn_ref[...], nt, preferred_element_type=F32) * scaling + bias
        high = jnp.maximum(
            jnp.max(s_past, axis=1, keepdims=True), jnp.max(s_new, axis=1, keepdims=True)
        )
        w_past = jnp.exp(s_past - high)
        w_new = jnp.exp(s_new - high)
        total = jnp.sum(w_past, axis=1, keepdims=True) + jnp.sum(w_new, axis=1, keepdims=True)
        num = jnp.dot(w_past.astype(BF16), vp_ref[...], preferred_element_type=F32) + jnp.dot(
            w_new.astype(BF16), vn_ref[...], preferred_element_type=F32
        )
        stat_lane = lax.broadcasted_iota(jnp.int32, (span, 128), 1)
        stats = jnp.where(stat_lane == 0, high, total).T
        line = jnp.concatenate([stats[i : i + 1, :] for i in range(2)], axis=1)
        coded = split_terms(line) + [jnp.zeros((stat_rows - 3, 2 * span), F32)]
        out[:span, :] = num.astype(BF16)
        out[span:, :] = jnp.concatenate(coded, axis=0).astype(BF16)

    attend(seq, num_all.at[seq])
    for frm in arrivals:
        src = rows_of(frm)
        remote(q_ref, qall.at[src], send_sem, q_rsem.at[frm], frm, rep).wait_recv()
        attend(frm, num_send.at[frm])
        send(num_send.at[frm], num_all.at[seq], num_rsem, frm, rep)

    wait_all(num_rsem, (n_seq - 1) * size_of(num_send.at[0]))

    lines = []
    for i in range(n_seq):
        coded = num_all[i, span:, :].astype(F32)
        lines.append(coded[0:1] + coded[1:2] + coded[2:3])
    lines.append(jnp.zeros((128 - n_seq, 2 * span), F32))
    stat_cols = jnp.concatenate(lines, axis=0).T
    highs = [stat_cols[:span, i : i + 1] for i in range(n_seq)]
    top = functools.reduce(jnp.maximum, highs)
    scales = [jnp.exp(h - top) for h in highs]
    full = sum(scales[i] * stat_cols[span:, i : i + 1] for i in range(n_seq))
    heads = sum(scales[i] * num_all[i, :span, :].astype(F32) for i in range(n_seq)) / full
    head_send[...] = heads.astype(BF16)

    def head_copy(to):
        return remote(head_send, head_all.at[seq], head_ssem, head_rsem.at[seq], rep, to)

    for j in range(1, chips):
        send(head_send, head_all.at[seq], head_rsem.at[seq], rep, same_core(j))
        send(head_send, head_all.at[seq], head_rsem.at[seq], rep, other_core(j))

    @pl.when(seq != rep)
    def _():
        head_copy(rep).start()

    send(head_send, head_all.at[seq], head_rsem.at[seq], rep, partner)
    loads[0].wait()

    def head_wait(f):
        remote(head_send, head_all.at[f], head_ssem, head_rsem.at[f], seq, rep).wait_recv()

    def project(f):
        block = jnp.concatenate(
            [head_all[f, h * tok : (h + 1) * tok, :] for h in range(q_per)], axis=1
        )
        part = jnp.dot(block, wproj[...], preferred_element_type=F32).astype(BF16)
        for t in range(n_seq):
            part_send[f, t] = part[:, t * slab : (t + 1) * slab]
        for to in far_first:
            send(part_send.at[f, to], part_all.at[seq, rows_of(f)], part_rsem, to, rep)
        part_all[seq, rows_of(f), :] = part_send[f, seq]

    @pl.when(seq == rep)
    def _():
        head_all[seq] = head_send[...]

    @pl.when(seq != rep)
    def _():
        head_wait(seq)

    project(seq)
    for f in arrivals:
        head_wait(f)
        project(f)

    wait_all(side_rsem, (n_seq - 1) * (tok * slab * 2 + tok * 128 * 4))

    @pl.when(seq != rep)
    def _():
        head_copy(rep).wait_send()

    wait_all(part_rsem, (n_seq - 1) * toks * slab * 2)
    summed = sum(part_all[f].astype(F32) for f in range(n_seq))
    xall[rep, seq] = (res_all[...].astype(F32) + summed).astype(BF16)

    def x_send(r, s, to_s, to_r):
        view = xall.at[r, s]
        send(view, view, x_rsem.at[r, s], to_s, to_r)

    def arrive(r, s):
        view = xall.at[r, s]
        remote(view, view, send_sem, x_rsem.at[r, s], seq, r).wait_recv()

    def spread(s, direct):
        for j in range(1, chips):
            x_send(rep, s, seq, same_core(j))
            if direct:
                x_send(rep, s, seq, other_core(j))
        x_send(rep, s, seq, partner)

    def from_seq(k):
        arrive(rep, arrivals[k])
        spread(arrivals[k], k > 0)

    def from_chip(s):
        for j in range(1, chips):
            arrive(same_core(j), s)
            x_send(same_core(j), s, seq, partner)

    spread(seq, False)
    for to in reversed(far_first):
        x_send(rep, seq, to, rep)
    hidden_width = wgate.shape[1]
    chunk = min(512, hidden_width)
    squares = [jnp.zeros((toks, 128), F32)]
    logits = [jnp.zeros((toks, router_split.shape[0]), F32)]

    def prepare(slots):
        for i, (r, s) in enumerate(slots):
            cols = pl.ds(pl.multiple_of(r * feat + s * slab, slab), slab)
            part = xall[r, s].astype(F32)
            squared = part * part
            for j in range(slab // 128):
                squares[0] = squares[0] + squared[:, j * 128 : (j + 1) * 128]
            scaled = (part * gain_ref[:, cols]).astype(BF16)
            gained[:, i * slab : (i + 1) * slab] = scaled
            logits[0] = logits[0] + lax.dot_general(
                scaled, router_split[:, cols], nt, preferred_element_type=F32
            )

    def products(slots, cols):
        total = None
        for i, (r, s) in enumerate(slots):
            span = pl.ds(pl.multiple_of(r * feat + s * slab, slab), slab)
            block = gained[:, i * slab : (i + 1) * slab]
            pair = (
                jnp.dot(block, wgate[span, cols], preferred_element_type=F32),
                jnp.dot(block, wup[span, cols], preferred_element_type=F32),
            )
            total = pair if total is None else (total[0] + pair[0], total[1] + pair[1])
        return total

    def add_slots(slots, start=False):
        prepare(slots)
        for c in range(hidden_width // chunk):
            cols = pl.ds(c * chunk, chunk)
            gate, up = products(slots, cols)
            if start:
                gate_acc[:, cols] = gate
                up_acc[:, cols] = up
            else:
                gate_acc[:, cols] += gate
                up_acc[:, cols] += up

    for load in loads[1:3]:
        load.wait()
    arrive(partner, seq)
    add_slots([(rep, seq), (partner, seq)], True)
    from_seq(0)
    from_chip(seq)
    from_seq(1)
    add_slots([(rep, arrivals[0]), (same_core(1), seq)])
    for k in range(2, n_seq - 1):
        from_seq(k)
    att_out[...] = jnp.concatenate([xall[rep, t, mine] for t in range(n_seq)], axis=1)
    arrive(partner, arrivals[0])
    arrive(other_core(1), seq)
    add_slots([(partner, arrivals[0]), (other_core(1), seq)])
    rest = arrivals[1:]
    add_slots([(rep, s) for s in rest])
    from_chip(arrivals[0])
    for s in rest:
        arrive(partner, s)
    add_slots([(partner, s) for s in rest])
    for s in rest[:-1]:
        arrive(same_core(1), s)
    add_slots([(same_core(1), s) for s in arrivals[:-1]])
    for s in arrivals[:-1]:
        arrive(other_core(1), s)
    add_slots([(other_core(1), s) for s in arrivals[:-1]])
    loads[3].wait()
    final = [(same_core(1), arrivals[-1]), (other_core(1), arrivals[-1])]
    for slot in final:
        arrive(*slot)
    prepare(final)
    square = jnp.sum(squares[0], axis=1, keepdims=True)
    inverse = lax.rsqrt(square / (feat * n_rep) + 1e-05)
    for c in range(hidden_width // chunk):
        cols = pl.ds(c * chunk, chunk)
        gate, up = products(final, cols)
        gate = (gate_acc[:, cols] + gate) * inverse
        up = (up_acc[:, cols] + up) * inverse
        hidden[:, cols] = (gate * jax.nn.sigmoid(gate) * up).astype(BF16)

    columns = [
        sum(logits[0][:, i * experts + e : i * experts + e + 1] for i in range(3)) * inverse
        for e in range(experts)
    ]
    first = [(idall[:, 0:1] == float(e)).astype(F32) for e in range(experts)]
    second = [(idall[:, 1:2] == float(e)).astype(F32) for e in range(experts)]
    gap = sum(first[e] * columns[e] for e in range(experts)) - sum(
        second[e] * columns[e] for e in range(experts)
    )
    share = jax.nn.sigmoid(gap)
    mine_first = (idall[:, 0:1] == (rep % experts).astype(F32)).astype(F32)
    mine_second = (idall[:, 1:2] == (rep % experts).astype(F32)).astype(F32)
    weight = share * mine_first + (1.0 - share) * mine_second

    def weighted(to, at, size):
        cols = pl.ds(pl.multiple_of(to * feat + at, size), size)
        return jnp.dot(hidden[...], wdown[:, cols], preferred_element_type=F32) * weight

    def cross(to_chip, h, parts):
        size = feat // parts
        cols = pl.ds(h * size, size)
        view = yall.at[to_chip, :, cols]
        ysend[to_chip, :, cols] = weighted(to_chip * 2 + 1 - core, h * size, size).astype(BF16)
        send(ysend.at[to_chip, :, cols], view, y_rsem.at[to_chip, h], seq, partner)

    def keep(to_chip, h, parts):
        size = feat // parts
        cols = pl.ds(h * size, size)
        owner = to_chip * 2 + core
        product = weighted(owner, h * size, size)
        view = yall.at[to_chip, :, cols]
        remote(view, view, send_sem, y_rsem.at[to_chip, h], seq, partner).wait_recv()
        psend[to_chip, :, cols] = (product + yall[to_chip, :, cols].astype(F32)).astype(BF16)
        place = fin_all.at[seq, chip, :, cols]
        for to in far_first:
            send(psend.at[to_chip, rows_of(to), cols], place, z_rsem.at[seq, chip], to, owner)

        @pl.when(chip != to_chip)
        def _():
            block = psend.at[to_chip, mine, cols]
            remote(block, place, send_sem, z_rsem.at[seq, chip], seq, owner).start()

    sent[0] += (chips - 1) * tok * feat * 2
    for to_chip in range(chips):
        parts = 1 if to_chip else HALF
        for h in range(parts):
            cross(to_chip, h, parts)
        for h in range(parts):
            keep(to_chip, h, parts)

    wait_all(cache_rsem, 2 * (n_rep - 1) * size_of(kn_ref))
    kc_out[...] = kcache[...]
    vc_out[...] = vcache[...]
    wait_all(cache_ssem, 2 * (n_rep - 1) * size_of(kn_ref))
    wait_all(send_sem, sent[0])

    result = att_out[...].astype(F32) + psend[chip, mine, :].astype(F32)
    for frm_s, frm_chip in [(seq, lax.rem(chip + j, chips)) for j in range(1, chips)] + [
        (s, lax.rem(chip + j, chips)) for s in arrivals for j in range(chips)
    ]:
        place = fin_all.at[frm_s, frm_chip]
        remote(place, place, send_sem, z_rsem.at[frm_s, frm_chip], frm_s, rep).wait_recv()
        result = result + fin_all[frm_s, frm_chip].astype(F32)
    layer_out[...] = result.astype(BF16)


def hand_over(*refs):
    sem = refs[8]
    copies = [pltpu.make_async_copy(refs[i], refs[4 + i], sem.at[i]) for i in range(4)]
    for copy in copies:
        copy.start()
    for copy in copies:
        copy.wait()


def fused_body(
    queries,
    keys_new,
    values_new,
    keys_past,
    values_past,
    block_order,
    residual,
    out_proj,
    norm_gain,
    router,
    w_gate,
    w_up,
    w_down,
    expert_ids,
):
    n_seq = lax.axis_size("seq")
    n_rep = lax.axis_size("rep")
    tok, width = queries.shape
    hd = keys_new.shape[1]
    toks = tok * n_seq
    rows = toks * (width // hd)
    feat = residual.shape[1]
    slab = feat // n_seq
    chips = n_rep // 2
    vmem = pl.BlockSpec(memory_space=pltpu.VMEM)
    hbm = pl.BlockSpec(memory_space=pl.ANY)
    dma = pltpu.SemaphoreType.DMA
    cache = (tok, hd * n_rep)
    outs = pl.pallas_call(
        functools.partial(fused_kernel, n_seq, n_rep),
        out_shape=(
            pltpu.VMEM((tok, feat), BF16),
            pltpu.VMEM((tok, feat), BF16),
            pltpu.VMEM(cache, BF16),
            pltpu.VMEM(cache, BF16),
        ),
        in_specs=[hbm] * 14,
        out_specs=(vmem,) * 4,
        scratch_shapes=[
            pltpu.SMEM(block_order.shape, jnp.int32),
            pltpu.VMEM(queries.shape, BF16),
            pltpu.VMEM(keys_new.shape, BF16),
            pltpu.VMEM(values_new.shape, BF16),
            pltpu.VMEM(keys_past.shape, BF16),
            pltpu.VMEM(values_past.shape, BF16),
            pltpu.VMEM(residual.shape, BF16),
            pltpu.VMEM((1, norm_gain.shape[0]), F32),
            pltpu.VMEM(router.shape[::-1], F32),
            pltpu.VMEM(expert_ids.shape[::-1], jnp.int32),
            dma((9,)),
            pltpu.VMEM(out_proj.shape, BF16),
            pltpu.VMEM(w_gate.shape[1:], BF16),
            pltpu.VMEM(w_up.shape[1:], BF16),
            pltpu.VMEM(w_down.shape[1:], BF16),
            pltpu.VMEM((toks, width), BF16),
            pltpu.VMEM((toks, 128), F32),
            pltpu.VMEM(cache, BF16),
            pltpu.VMEM(cache, BF16),
            pltpu.VMEM((n_seq, rows // n_seq + 16, hd), BF16),
            pltpu.VMEM((n_seq, rows // n_seq + 16, hd), BF16),
            pltpu.VMEM((rows // n_seq, hd), BF16),
            pltpu.VMEM((n_seq, rows // n_seq, hd), BF16),
            pltpu.VMEM((toks, slab), BF16),
            pltpu.VMEM((n_seq, n_seq, tok, slab), BF16),
            pltpu.VMEM((n_seq, toks, slab), BF16),
            pltpu.VMEM((n_rep, n_seq, toks, slab), BF16),
            pltpu.VMEM((toks, (n_seq - 2) * slab), BF16),
            pltpu.VMEM((16, norm_gain.shape[0]), BF16),
            pltpu.VMEM((toks, w_gate.shape[2]), F32),
            pltpu.VMEM((toks, w_gate.shape[2]), F32),
            pltpu.VMEM((toks, w_gate.shape[2]), BF16),
            pltpu.VMEM((chips, toks, feat), BF16),
            pltpu.VMEM((chips, toks, feat), BF16),
            pltpu.VMEM((chips, toks, feat), BF16),
            pltpu.VMEM((n_seq, chips, tok, feat), BF16),
            dma((4,)),
            dma((n_seq,)),
            dma,
            dma,
            dma,
            dma,
            dma,
            dma((n_seq,)),
            dma,
            dma((n_rep, n_seq)),
            dma((chips, HALF)),
            dma((n_seq, chips)),
            dma,
        ],
        compiler_params=pltpu.CompilerParams(
            collective_id=0, has_side_effects=True, vmem_limit_bytes=62 * 1024 * 1024
        ),
    )(
        block_order,
        queries,
        keys_new,
        values_new,
        keys_past,
        values_past,
        residual,
        norm_gain.reshape(1, -1),
        router.T,
        expert_ids.T,
        out_proj,
        w_gate,
        w_up,
        w_down,
    )
    return pl.pallas_call(
        hand_over,
        out_shape=tuple(jax.ShapeDtypeStruct(out.shape, out.dtype) for out in outs),
        in_specs=[hbm] * 4,
        out_specs=(hbm,) * 4,
        scratch_shapes=[dma((4,))],
    )(*[pltpu.with_memory_space_constraint(out, pltpu.VMEM) for out in outs])


def body(*arrays):
    queries, out_proj = arrays[0], arrays[7]
    n_seq, n_rep = lax.axis_size("seq"), lax.axis_size("rep")
    held = 2 * sum(math.prod(array.shape) for array in arrays[10:13])
    tok, width, hd = queries.shape[0], queries.shape[1], arrays[1].shape[1]
    fits = held <= 50 * 1024 * 1024 and n_seq == n_rep and n_rep == 4
    fits = fits and 2 * tok * (width // hd) == hd == 128 and tok % 16 == 0
    if fits and out_proj.shape[0] == queries.shape[1]:
        return fused_body(*arrays)
    return plain_body(*arrays)


def solution(mesh):
    in_specs = (
        P(("groups", "seq"), "rep"),
        P(("groups", "seq"), "rep"),
        P(("groups", "seq"), "rep"),
        P(("groups", "seq"), "rep"),
        P(("groups", "seq"), "rep"),
        P("groups"),
        P(("groups", "seq"), "rep"),
        P("seq", "rep"),
        P(),
        P(),
        P("rep", None, "seq"),
        P("rep", None, "seq"),
        P("rep", "seq", None),
        P(("groups", "seq"), None),
    )
    out_specs = (
        P(("groups", "seq"), "rep"),
        P(("groups", "seq"), "rep"),
        P(("groups", "seq"), None),
        P(("groups", "seq"), None),
    )
    return jax.shard_map(body, mesh=mesh, in_specs=in_specs, out_specs=out_specs, check_vma=False)
```

```python
import functools
import math

import jax
import jax.numpy as jnp
from jax import lax
from jax.experimental import pallas as pl
from jax.experimental.pallas import tpu as pltpu
from jax.sharding import PartitionSpec as P

EXPERTS = 4
CAP = 12


def block_lookup(owners, block_order):
    width = block_order.shape[0]
    hits = owners[:, None] == jnp.arange(width, dtype=jnp.int32)[None, :]
    return jnp.sum(jnp.where(hits, block_order[None, :], 0), axis=1)


def plain_body(
    queries,
    keys_new,
    values_new,
    keys_past,
    values_past,
    block_order,
    residual,
    out_proj,
    norm_gain,
    router,
    w_gate,
    w_up,
    w_down,
    expert_ids,
):
    seq_index = lax.axis_index("seq")
    rep_index = lax.axis_index("rep")
    rep_count = lax.axis_size("rep")
    tok_count = queries.shape[0]
    head_dim = keys_new.shape[1]
    q_per = queries.shape[1] // head_dim
    past_len = keys_past.shape[0]
    key_span = past_len + tok_count
    row_total = tok_count * q_per
    my_block = block_lookup(jnp.full((1,), seq_index, jnp.int32), block_order)[0]
    scaling = 1.0 / math.sqrt(head_dim)
    query_rows = queries.reshape(row_total, head_dim)
    query_pos = my_block * tok_count + jnp.arange(row_total, dtype=jnp.int32) // q_per
    keys_local = jnp.concatenate([keys_past, keys_new], axis=0)
    values_local = jnp.concatenate([values_past, values_new], axis=0)
    running = jnp.full((row_total,), -1e30, jnp.float32)
    key_piece = lax.all_gather(keys_local, "seq", axis=0, tiled=True)
    value_piece = lax.all_gather(values_local, "seq", axis=0, tiled=True)
    row_count = key_piece.shape[0]
    key_index = jnp.arange(row_count, dtype=jnp.int32)
    key_owner = key_index // key_span
    offset = key_index % key_span
    key_pos = block_lookup(key_owner, block_order) * tok_count + offset - past_len
    visible = (offset < past_len)[None, :] | (key_pos[None, :] <= query_pos[:, None])
    scores = jnp.dot(query_rows, key_piece.T, preferred_element_type=jnp.float32) * scaling
    highest = jnp.maximum(running, jnp.max(jnp.where(visible, scores, -1e30), axis=1))
    weights = jnp.where(visible, jnp.exp(scores - highest[:, None]), 0.0)
    totals = jnp.sum(weights, axis=1)
    numerator = jnp.dot(
        weights.astype(jnp.bfloat16), value_piece, preferred_element_type=jnp.float32
    )
    running, totals, numerator = (highest, totals, numerator)
    attn_local = (
        (numerator / totals[:, None]).reshape(tok_count, q_per * head_dim).astype(jnp.bfloat16)
    )
    attn_full, keys_cache, values_cache = (
        lax.all_gather(attn_local, "rep", axis=1, tiled=True),
        lax.all_gather(keys_new, "rep", axis=1, tiled=True),
        lax.all_gather(values_new, "rep", axis=1, tiled=True),
    )
    head_rows = lax.all_to_all(attn_full, "seq", split_axis=1, concat_axis=0, tiled=True)
    projected = lax.psum_scatter(
        jnp.dot(head_rows, out_proj, preferred_element_type=jnp.float32).astype(jnp.bfloat16),
        "seq",
        scatter_dimension=0,
        tiled=True,
    ).astype(jnp.float32)
    attended = (residual.astype(jnp.float32) + projected).astype(jnp.bfloat16)
    full_rows = lax.all_gather(attended, "rep", axis=1, tiled=True)
    features = full_rows.astype(jnp.float32)
    mean_square = jnp.mean(features * features, axis=1, keepdims=True)
    normed = (features * norm_gain[None, :] * lax.rsqrt(mean_square + 1e-05)).astype(jnp.bfloat16)
    logits = jnp.dot(normed.astype(jnp.float32), router, precision=lax.Precision.HIGHEST)
    expert_range = jnp.arange(EXPERTS, dtype=jnp.int32)
    first_pick = (expert_ids[:, 0:1] == expert_range[None, :]).astype(jnp.float32)
    second_pick = (expert_ids[:, 1:2] == expert_range[None, :]).astype(jnp.float32)
    share_first = jax.nn.sigmoid(
        jnp.sum(first_pick * logits, axis=1) - jnp.sum(second_pick * logits, axis=1)
    )
    token_share = share_first[:, None] * first_pick + (1.0 - share_first)[:, None] * second_pick
    member = first_pick + second_pick
    ranking = jnp.cumsum(member, axis=0) - member
    slot_range = jnp.arange(CAP, dtype=jnp.float32)
    selection = member.T[:, None, :] * (ranking.T[:, None, :] == slot_range[None, :, None]).astype(
        jnp.float32
    )
    mine_mask = (expert_range == rep_index % EXPERTS).astype(jnp.float32)
    my_selection = jnp.einsum("e,ejt->jt", mine_mask, selection)
    slot_rows = jnp.dot(
        my_selection.astype(jnp.bfloat16), normed, preferred_element_type=jnp.float32
    ).astype(jnp.bfloat16)
    gate_local = w_gate[0]
    up_local = w_up[0]
    down_local = w_down[0]
    piece = lax.all_gather(slot_rows, "seq", axis=0, tiled=True)
    gate_part = jnp.dot(piece, gate_local, preferred_element_type=jnp.float32)
    up_part = jnp.dot(piece, up_local, preferred_element_type=jnp.float32)
    hidden_slots = (jax.nn.silu(gate_part) * up_part).astype(jnp.bfloat16)
    expert_part = lax.psum_scatter(
        jnp.dot(hidden_slots, down_local, preferred_element_type=jnp.float32).astype(jnp.bfloat16),
        "seq",
        scatter_dimension=0,
        tiled=True,
    ).astype(jnp.float32)
    returned = lax.all_to_all(
        expert_part.astype(jnp.bfloat16), "rep", split_axis=1, concat_axis=0, tiled=True
    ).astype(expert_part.dtype)
    source_expert = jnp.arange(rep_count, dtype=jnp.int32) % EXPERTS
    source_pick = (source_expert[:, None] == expert_range[None, :]).astype(jnp.float32)
    combine = jnp.einsum("re,ejt,te->trj", source_pick, selection, token_share).reshape(
        tok_count, rep_count * CAP
    )
    moe_slice = jnp.dot(combine, returned, precision=lax.Precision.HIGHEST)
    layer_out = (attended.astype(jnp.float32) + moe_slice).astype(jnp.bfloat16)
    return (attended, layer_out, keys_cache, values_cache)


MESH = pl.DeviceIdType.MESH
HALF = 2
F32 = jnp.float32
BF16 = jnp.bfloat16


def fused_kernel(
    n_seq,
    n_rep,
    order_hbm,
    q_hbm,
    kn_hbm,
    vn_hbm,
    kp_hbm,
    vp_hbm,
    res_hbm,
    gain_hbm,
    router_hbm,
    ids_hbm,
    proj_hbm,
    gate_hbm,
    up_hbm,
    down_hbm,
    att_out,
    layer_out,
    kc_out,
    vc_out,
    order_ref,
    q_ref,
    kn_ref,
    vn_ref,
    kp_ref,
    vp_ref,
    res_ref,
    gain_ref,
    router_ref,
    ids_ref,
    in_sem,
    wproj,
    wgate,
    wup,
    wdown,
    qall,
    idall,
    kcache,
    vcache,
    num_send,
    num_all,
    head_send,
    head_all,
    res_all,
    part_send,
    part_all,
    xall,
    gained,
    router_split,
    gate_acc,
    up_acc,
    hidden,
    ysend,
    yall,
    psend,
    fin_all,
    w_sem,
    q_rsem,
    side_rsem,
    cache_rsem,
    cache_ssem,
    num_rsem,
    head_ssem,
    head_rsem,
    part_rsem,
    x_rsem,
    y_rsem,
    z_rsem,
    send_sem,
):
    group = lax.axis_index("groups")
    seq = lax.axis_index("seq")
    rep = lax.axis_index("rep")
    tok, width = q_ref.shape
    hd = kn_ref.shape[1]
    q_per = width // hd
    toks = tok * n_seq
    feat = res_ref.shape[1]
    slab = feat // n_seq
    stat_rows = num_send.shape[1] - tok * q_per

    chips = n_rep // 2
    chip, core = rep // 2, lax.rem(rep, 2)
    partner = chip * 2 + 1 - core

    def same_core(step):
        return lax.rem(chip + step, chips) * 2 + core

    def other_core(step):
        return lax.rem(chip + step, chips) * 2 + 1 - core

    def dev(s, r):
        return {"groups": group, "seq": s, "rep": r}

    def other(index, step, size):
        return lax.rem(index + step, size)

    def remote(src, dst, ssem, rsem, s, r):
        return pltpu.make_async_remote_copy(
            src_ref=src,
            dst_ref=dst,
            send_sem=ssem,
            recv_sem=rsem,
            device_id=dev(s, r),
            device_id_type=MESH,
        )

    def rows_of(index):
        return pl.ds(pl.multiple_of(index * tok, tok), tok)

    def split_terms(rest):
        terms = []
        for _ in range(3):
            terms.append(rest.astype(BF16).astype(F32))
            rest = rest - terms[-1]
        return terms

    def size_of(ref):
        return math.prod(ref.shape) * ref.dtype.itemsize

    def wait_all(sem, size):
        tiles = size // (16 * 128 * 2)
        wide = max(w for w in range(1, wgate.shape[1] // 128 + 1) if tiles % w == 0)
        span = wgate.at[pl.ds(0, tiles // wide * 16), pl.ds(0, wide * 128)]
        pltpu.make_async_copy(span, span, sem).wait()

    def slab_of(index):
        return pl.ds(pl.multiple_of(index * slab, slab), slab)

    def per_seq(rows):
        return [sum(jnp.where(seq == s, rows[s][k], 0) for s in range(n_seq)) for k in range(n_seq - 1)]

    def others(s):
        return [t for t in range(n_seq) if t != s]

    far_first = per_seq([sorted(others(s), key=lambda t: -abs(t - s)) for s in range(n_seq)])
    arrivals = per_seq(
        [
            sorted(others(s), key=lambda f: (abs(f - s), f if 2 * s < n_seq else -f))
            for s in range(n_seq)
        ]
    )

    smalls = [
        pltpu.make_async_copy(src, dst, in_sem.at[(0, 1, 2, 2, 3, 3, 4, 5, 6, 7)[i]])
        for i, (src, dst) in enumerate(
            (
                (ids_hbm, ids_ref),
                (q_hbm, q_ref),
                (kn_hbm, kn_ref),
                (vn_hbm, vn_ref),
                (kp_hbm, kp_ref),
                (vp_hbm, vp_ref),
                (order_hbm, order_ref),
                (res_hbm, res_ref),
                (gain_hbm, gain_ref),
                (router_hbm, router_ref),
            )
        )
    ]
    for small in smalls:
        small.start()

    barrier = pltpu.get_barrier_semaphore()
    for i in reversed(range(n_seq)):
        for j in reversed(range(n_rep)):
            if i or j:
                pl.semaphore_signal(
                    barrier,
                    inc=1,
                    device_id=dev(other(seq, i, n_seq), other(rep, j, n_rep)),
                    device_id_type=MESH,
                )

    loads = []
    for i, (src, dst) in enumerate(
        ((proj_hbm, wproj), (gate_hbm.at[0], wgate), (up_hbm.at[0], wup), (down_hbm.at[0], wdown))
    ):
        pieces = 1 if i == 0 else 4
        size = dst.shape[0] // pieces
        for j in range(pieces):
            span = pl.ds(j * size, size)
            pltpu.make_async_copy(src.at[span], dst.at[span], w_sem.at[i]).start()
        loads.append(pltpu.make_async_copy(src, dst, w_sem.at[i]))

    smalls[0].wait()
    smalls[1].wait()
    wait_all(in_sem.at[2], 2 * size_of(kn_ref))
    lane = lax.broadcasted_iota(jnp.int32, (tok, 128), 1)
    ids_f = ids_ref[...].astype(F32)
    diagonal = lax.broadcasted_iota(jnp.int32, (tok, tok), 0) == lax.broadcasted_iota(
        jnp.int32, (tok, tok), 1
    )
    picks = [
        jnp.sum(jnp.where(diagonal, ids_f[i : i + 1, :], 0.0), axis=1, keepdims=True)
        for i in range(2)
    ]
    idall[rows_of(seq), :] = jnp.where(lane == 0, picks[0], picks[1])
    qall[rows_of(seq), :] = q_ref[...]
    for j in range(n_rep):

        @pl.when(rep == j)
        def _():
            kcache[:, j * hd : (j + 1) * hd] = kn_ref[...]
            vcache[:, j * hd : (j + 1) * hd] = vn_ref[...]

    pl.semaphore_wait(barrier, n_seq * n_rep - 1)

    sent = [0]

    def send(ref, *rest):
        sent[0] += size_of(ref)
        remote(ref, rest[0], send_sem, *rest[1:]).start()

    mine = rows_of(seq)
    for to in far_first:
        send(q_ref, qall.at[mine], q_rsem.at[seq], to, rep)

    experts = router_ref.shape[0]
    wait_all(in_sem.at[3], 2 * size_of(kp_ref))
    for small in smalls[6:]:
        small.wait()
    own_pos = order_ref[seq] * tok + lax.broadcasted_iota(jnp.int32, (tok, tok), 1)
    terms = split_terms(router_ref[...])
    terms.append(jnp.zeros((router_split.shape[0] - 3 * experts, router_ref.shape[1]), F32))
    router_split[...] = jnp.concatenate(terms, axis=0).astype(BF16)
    for to in far_first:
        send(res_ref.at[:, slab_of(to)], res_all.at[mine], side_rsem, to, rep)
        send(idall.at[mine], idall.at[mine], side_rsem, to, rep)
    res_all[mine, :] = res_ref[:, slab_of(seq)]
    for j in range(n_rep):

        @pl.when(rep == j)
        def _():
            cols = pl.ds(j * hd, hd)
            for k in range(1, n_rep):
                to = (j + k) % n_rep
                remote(kn_ref, kcache.at[:, cols], cache_ssem, cache_rsem, seq, to).start()
                remote(vn_ref, vcache.at[:, cols], cache_ssem, cache_rsem, seq, to).start()

    scaling = 1.0 / math.sqrt(hd)
    nt = (((1,), (1,)), ((), ()))
    span = tok * q_per
    row = lax.broadcasted_iota(jnp.int32, (tok, tok), 0)

    def attend(t, out):
        block = qall[rows_of(t), :]
        block = jnp.concatenate([block[:, h * hd : (h + 1) * hd] for h in range(q_per)], axis=0)
        bias = jnp.where(own_pos <= order_ref[t] * tok + row, 0.0, -1e30)
        bias = jnp.concatenate([bias] * q_per, axis=0)
        s_past = lax.dot_general(block, kp_ref[...], nt, preferred_element_type=F32) * scaling
        s_new = lax.dot_general(block, kn_ref[...], nt, preferred_element_type=F32) * scaling + bias
        high = jnp.maximum(
            jnp.max(s_past, axis=1, keepdims=True), jnp.max(s_new, axis=1, keepdims=True)
        )
        w_past = jnp.exp(s_past - high)
        w_new = jnp.exp(s_new - high)
        total = jnp.sum(w_past, axis=1, keepdims=True) + jnp.sum(w_new, axis=1, keepdims=True)
        num = jnp.dot(w_past.astype(BF16), vp_ref[...], preferred_element_type=F32) + jnp.dot(
            w_new.astype(BF16), vn_ref[...], preferred_element_type=F32
        )
        stat_lane = lax.broadcasted_iota(jnp.int32, (span, 128), 1)
        stats = jnp.where(stat_lane == 0, high, total).T
        line = jnp.concatenate([stats[i : i + 1, :] for i in range(2)], axis=1)
        coded = split_terms(line) + [jnp.zeros((stat_rows - 3, 2 * span), F32)]
        out[:span, :] = num.astype(BF16)
        out[span:, :] = jnp.concatenate(coded, axis=0).astype(BF16)

    attend(seq, num_all.at[seq])
    for frm in arrivals:
        src = rows_of(frm)
        remote(q_ref, qall.at[src], send_sem, q_rsem.at[frm], frm, rep).wait_recv()
        attend(frm, num_send.at[frm])
        send(num_send.at[frm], num_all.at[seq], num_rsem, frm, rep)

    wait_all(num_rsem, (n_seq - 1) * size_of(num_send.at[0]))

    ones = jnp.where(lax.broadcasted_iota(jnp.int32, (stat_rows, hd), 0) < 3, 1.0, 0.0).astype(BF16)
    tn = (((0,), (0,)), ((), ()))
    stat_cols = [
        lax.dot_general(num_all[i, span:, :], ones, tn, preferred_element_type=F32)
        for i in range(n_seq)
    ]
    highs = [cols[:span] for cols in stat_cols]
    top = functools.reduce(jnp.maximum, highs)
    scales = [jnp.exp(h - top) for h in highs]
    full = sum(scales[i] * stat_cols[i][span:] for i in range(n_seq))
    heads = sum(scales[i] * num_all[i, :span, :].astype(F32) for i in range(n_seq)) / full
    head_send[...] = heads.astype(BF16)

    def head_copy(to):
        return remote(head_send, head_all.at[seq], head_ssem, head_rsem.at[seq], rep, to)

    for j in range(1, chips):
        send(head_send, head_all.at[seq], head_rsem.at[seq], rep, same_core(j))
        send(head_send, head_all.at[seq], head_rsem.at[seq], rep, other_core(j))

    @pl.when(seq != rep)
    def _():
        head_copy(rep).start()

    send(head_send, head_all.at[seq], head_rsem.at[seq], rep, partner)
    loads[0].wait()

    def head_wait(f):
        remote(head_send, head_all.at[f], head_ssem, head_rsem.at[f], seq, rep).wait_recv()

    def project(f):
        block = jnp.concatenate(
            [head_all[f, h * tok : (h + 1) * tok, :] for h in range(q_per)], axis=1
        )
        part = jnp.dot(block, wproj[...], preferred_element_type=F32).astype(BF16)
        for t in range(n_seq):
            part_send[f, t] = part[:, t * slab : (t + 1) * slab]
        for to in far_first:
            send(part_send.at[f, to], part_all.at[seq, rows_of(f)], part_rsem, to, rep)
        part_all[seq, rows_of(f), :] = part_send[f, seq]

    @pl.when(seq == rep)
    def _():
        head_all[seq] = head_send[...]

    @pl.when(seq != rep)
    def _():
        head_wait(seq)

    project(seq)
    for f in arrivals:
        head_wait(f)
        project(f)

    wait_all(side_rsem, (n_seq - 1) * (tok * slab * 2 + tok * 128 * 4))

    @pl.when(seq != rep)
    def _():
        head_copy(rep).wait_send()

    wait_all(part_rsem, (n_seq - 1) * toks * slab * 2)
    summed = sum(part_all[f].astype(F32) for f in range(n_seq))
    xall[rep, seq] = (res_all[...].astype(F32) + summed).astype(BF16)

    def x_send(r, s, to_s, to_r):
        view = xall.at[r, s]
        send(view, view, x_rsem.at[r, s], to_s, to_r)

    def arrive(r, s):
        view = xall.at[r, s]
        remote(view, view, send_sem, x_rsem.at[r, s], seq, r).wait_recv()

    def spread(s, direct):
        for j in range(1, chips):
            x_send(rep, s, seq, same_core(j))
            if direct:
                x_send(rep, s, seq, other_core(j))
        x_send(rep, s, seq, partner)

    def from_seq(k):
        arrive(rep, arrivals[k])
        spread(arrivals[k], k > 0)

    def from_chip(s):
        for j in range(1, chips):
            arrive(same_core(j), s)
            x_send(same_core(j), s, seq, partner)

    spread(seq, False)
    for to in reversed(far_first):
        x_send(rep, seq, to, rep)
    hidden_width = wgate.shape[1]
    chunk = min(512, hidden_width)
    squares = [jnp.zeros((toks, 128), F32)]
    logits = [jnp.zeros((toks, router_split.shape[0]), F32)]

    def prepare(slots):
        for i, (r, s) in enumerate(slots):
            cols = pl.ds(pl.multiple_of(r * feat + s * slab, slab), slab)
            part = xall[r, s].astype(F32)
            squared = part * part
            for j in range(slab // 128):
                squares[0] = squares[0] + squared[:, j * 128 : (j + 1) * 128]
            scaled = (part * gain_ref[:, cols]).astype(BF16)
            gained[:, i * slab : (i + 1) * slab] = scaled
            logits[0] = logits[0] + lax.dot_general(
                scaled, router_split[:, cols], nt, preferred_element_type=F32
            )

    def products(slots, cols):
        total = None
        for i, (r, s) in enumerate(slots):
            span = pl.ds(pl.multiple_of(r * feat + s * slab, slab), slab)
            block = gained[:, i * slab : (i + 1) * slab]
            pair = (
                jnp.dot(block, wgate[span, cols], preferred_element_type=F32),
                jnp.dot(block, wup[span, cols], preferred_element_type=F32),
            )
            total = pair if total is None else (total[0] + pair[0], total[1] + pair[1])
        return total

    def add_slots(slots, start=False):
        prepare(slots)
        for c in range(hidden_width // chunk):
            cols = pl.ds(c * chunk, chunk)
            gate, up = products(slots, cols)
            if start:
                gate_acc[:, cols] = gate
                up_acc[:, cols] = up
            else:
                gate_acc[:, cols] += gate
                up_acc[:, cols] += up

    for load in loads[1:3]:
        load.wait()
    arrive(partner, seq)
    add_slots([(rep, seq), (partner, seq)], True)
    from_seq(0)
    from_chip(seq)
    from_seq(1)
    add_slots([(rep, arrivals[0]), (same_core(1), seq)])
    for k in range(2, n_seq - 1):
        from_seq(k)
    att_out[...] = jnp.concatenate([xall[rep, t, mine] for t in range(n_seq)], axis=1)
    arrive(partner, arrivals[0])
    arrive(other_core(1), seq)
    add_slots([(partner, arrivals[0]), (other_core(1), seq)])
    rest = arrivals[1:]
    add_slots([(rep, s) for s in rest])
    from_chip(arrivals[0])
    for s in rest:
        arrive(partner, s)
    add_slots([(partner, s) for s in rest])
    for s in rest[:-1]:
        arrive(same_core(1), s)
    add_slots([(same_core(1), s) for s in arrivals[:-1]])
    for s in arrivals[:-1]:
        arrive(other_core(1), s)
    add_slots([(other_core(1), s) for s in arrivals[:-1]])
    loads[3].wait()
    final = [(same_core(1), arrivals[-1]), (other_core(1), arrivals[-1])]
    for slot in final:
        arrive(*slot)
    prepare(final)
    square = jnp.sum(squares[0], axis=1, keepdims=True)
    inverse = lax.rsqrt(square / (feat * n_rep) + 1e-05)
    for c in range(hidden_width // chunk):
        cols = pl.ds(c * chunk, chunk)
        gate, up = products(final, cols)
        gate = (gate_acc[:, cols] + gate) * inverse
        up = (up_acc[:, cols] + up) * inverse
        hidden[:, cols] = (gate * jax.nn.sigmoid(gate) * up).astype(BF16)

    columns = [
        sum(logits[0][:, i * experts + e : i * experts + e + 1] for i in range(3)) * inverse
        for e in range(experts)
    ]
    first = [(idall[:, 0:1] == float(e)).astype(F32) for e in range(experts)]
    second = [(idall[:, 1:2] == float(e)).astype(F32) for e in range(experts)]
    gap = sum(first[e] * columns[e] for e in range(experts)) - sum(
        second[e] * columns[e] for e in range(experts)
    )
    share = jax.nn.sigmoid(gap)
    mine_first = (idall[:, 0:1] == (rep % experts).astype(F32)).astype(F32)
    mine_second = (idall[:, 1:2] == (rep % experts).astype(F32)).astype(F32)
    weight = share * mine_first + (1.0 - share) * mine_second

    def weighted(to, at, size):
        cols = pl.ds(pl.multiple_of(to * feat + at, size), size)
        return jnp.dot(hidden[...], wdown[:, cols], preferred_element_type=F32) * weight

    def cross(to_chip, h, parts):
        size = feat // parts
        cols = pl.ds(h * size, size)
        view = yall.at[to_chip, :, cols]
        ysend[to_chip, :, cols] = weighted(to_chip * 2 + 1 - core, h * size, size).astype(BF16)
        send(ysend.at[to_chip, :, cols], view, y_rsem.at[to_chip, h], seq, partner)

    def keep(to_chip, h, parts):
        size = feat // parts
        cols = pl.ds(h * size, size)
        owner = to_chip * 2 + core
        product = weighted(owner, h * size, size)
        view = yall.at[to_chip, :, cols]
        remote(view, view, send_sem, y_rsem.at[to_chip, h], seq, partner).wait_recv()
        psend[to_chip, :, cols] = (product + yall[to_chip, :, cols].astype(F32)).astype(BF16)
        place = fin_all.at[seq, chip, :, cols]
        for to in far_first:
            send(psend.at[to_chip, rows_of(to), cols], place, z_rsem.at[seq, chip], to, owner)

        @pl.when(chip != to_chip)
        def _():
            block = psend.at[to_chip, mine, cols]
            remote(block, place, send_sem, z_rsem.at[seq, chip], seq, owner).start()

    sent[0] += (chips - 1) * tok * feat * 2
    for to_chip in range(chips):
        parts = 1 if to_chip else HALF
        for h in range(parts):
            cross(to_chip, h, parts)
        for h in range(parts):
            keep(to_chip, h, parts)

    wait_all(cache_rsem, 2 * (n_rep - 1) * size_of(kn_ref))
    kc_out[...] = kcache[...]
    vc_out[...] = vcache[...]
    wait_all(cache_ssem, 2 * (n_rep - 1) * size_of(kn_ref))
    wait_all(send_sem, sent[0])

    result = att_out[...].astype(F32) + psend[chip, mine, :].astype(F32)
    for frm_s, frm_chip in [(seq, lax.rem(chip + j, chips)) for j in range(1, chips)] + [
        (s, lax.rem(chip + j, chips)) for s in arrivals for j in range(chips)
    ]:
        place = fin_all.at[frm_s, frm_chip]
        remote(place, place, send_sem, z_rsem.at[frm_s, frm_chip], frm_s, rep).wait_recv()
        result = result + fin_all[frm_s, frm_chip].astype(F32)
    layer_out[...] = result.astype(BF16)


def hand_over(*refs):
    sem = refs[8]
    copies = [pltpu.make_async_copy(refs[i], refs[4 + i], sem.at[i]) for i in range(4)]
    for copy in copies:
        copy.start()
    for copy in copies:
        copy.wait()


def fused_body(
    queries,
    keys_new,
    values_new,
    keys_past,
    values_past,
    block_order,
    residual,
    out_proj,
    norm_gain,
    router,
    w_gate,
    w_up,
    w_down,
    expert_ids,
):
    n_seq = lax.axis_size("seq")
    n_rep = lax.axis_size("rep")
    tok, width = queries.shape
    hd = keys_new.shape[1]
    toks = tok * n_seq
    rows = toks * (width // hd)
    feat = residual.shape[1]
    slab = feat // n_seq
    chips = n_rep // 2
    vmem = pl.BlockSpec(memory_space=pltpu.VMEM)
    hbm = pl.BlockSpec(memory_space=pl.ANY)
    dma = pltpu.SemaphoreType.DMA
    cache = (tok, hd * n_rep)
    outs = pl.pallas_call(
        functools.partial(fused_kernel, n_seq, n_rep),
        out_shape=(
            pltpu.VMEM((tok, feat), BF16),
            pltpu.VMEM((tok, feat), BF16),
            pltpu.VMEM(cache, BF16),
            pltpu.VMEM(cache, BF16),
        ),
        in_specs=[hbm] * 14,
        out_specs=(vmem,) * 4,
        scratch_shapes=[
            pltpu.SMEM(block_order.shape, jnp.int32),
            pltpu.VMEM(queries.shape, BF16),
            pltpu.VMEM(keys_new.shape, BF16),
            pltpu.VMEM(values_new.shape, BF16),
            pltpu.VMEM(keys_past.shape, BF16),
            pltpu.VMEM(values_past.shape, BF16),
            pltpu.VMEM(residual.shape, BF16),
            pltpu.VMEM((1, norm_gain.shape[0]), F32),
            pltpu.VMEM(router.shape[::-1], F32),
            pltpu.VMEM(expert_ids.shape[::-1], jnp.int32),
            dma((9,)),
            pltpu.VMEM(out_proj.shape, BF16),
            pltpu.VMEM(w_gate.shape[1:], BF16),
            pltpu.VMEM(w_up.shape[1:], BF16),
            pltpu.VMEM(w_down.shape[1:], BF16),
            pltpu.VMEM((toks, width), BF16),
            pltpu.VMEM((toks, 128), F32),
            pltpu.VMEM(cache, BF16),
            pltpu.VMEM(cache, BF16),
            pltpu.VMEM((n_seq, rows // n_seq + 16, hd), BF16),
            pltpu.VMEM((n_seq, rows // n_seq + 16, hd), BF16),
            pltpu.VMEM((rows // n_seq, hd), BF16),
            pltpu.VMEM((n_seq, rows // n_seq, hd), BF16),
            pltpu.VMEM((toks, slab), BF16),
            pltpu.VMEM((n_seq, n_seq, tok, slab), BF16),
            pltpu.VMEM((n_seq, toks, slab), BF16),
            pltpu.VMEM((n_rep, n_seq, toks, slab), BF16),
            pltpu.VMEM((toks, (n_seq - 2) * slab), BF16),
            pltpu.VMEM((16, norm_gain.shape[0]), BF16),
            pltpu.VMEM((toks, w_gate.shape[2]), F32),
            pltpu.VMEM((toks, w_gate.shape[2]), F32),
            pltpu.VMEM((toks, w_gate.shape[2]), BF16),
            pltpu.VMEM((chips, toks, feat), BF16),
            pltpu.VMEM((chips, toks, feat), BF16),
            pltpu.VMEM((chips, toks, feat), BF16),
            pltpu.VMEM((n_seq, chips, tok, feat), BF16),
            dma((4,)),
            dma((n_seq,)),
            dma,
            dma,
            dma,
            dma,
            dma,
            dma((n_seq,)),
            dma,
            dma((n_rep, n_seq)),
            dma((chips, HALF)),
            dma((n_seq, chips)),
            dma,
        ],
        compiler_params=pltpu.CompilerParams(
            collective_id=0, has_side_effects=True, vmem_limit_bytes=62 * 1024 * 1024
        ),
    )(
        block_order,
        queries,
        keys_new,
        values_new,
        keys_past,
        values_past,
        residual,
        norm_gain.reshape(1, -1),
        router.T,
        expert_ids.T,
        out_proj,
        w_gate,
        w_up,
        w_down,
    )
    return pl.pallas_call(
        hand_over,
        out_shape=tuple(jax.ShapeDtypeStruct(out.shape, out.dtype) for out in outs),
        in_specs=[hbm] * 4,
        out_specs=(hbm,) * 4,
        scratch_shapes=[dma((4,))],
    )(*[pltpu.with_memory_space_constraint(out, pltpu.VMEM) for out in outs])


def body(*arrays):
    queries, out_proj = arrays[0], arrays[7]
    n_seq, n_rep = lax.axis_size("seq"), lax.axis_size("rep")
    held = 2 * sum(math.prod(array.shape) for array in arrays[10:13])
    tok, width, hd = queries.shape[0], queries.shape[1], arrays[1].shape[1]
    fits = held <= 50 * 1024 * 1024 and n_seq == n_rep and n_rep == 4
    fits = fits and 2 * tok * (width // hd) == hd == 128 and tok % 16 == 0
    if fits and out_proj.shape[0] == queries.shape[1]:
        return fused_body(*arrays)
    return plain_body(*arrays)


def solution(mesh):
    in_specs = (
        P(("groups", "seq"), "rep"),
        P(("groups", "seq"), "rep"),
        P(("groups", "seq"), "rep"),
        P(("groups", "seq"), "rep"),
        P(("groups", "seq"), "rep"),
        P("groups"),
        P(("groups", "seq"), "rep"),
        P("seq", "rep"),
        P(),
        P(),
        P("rep", None, "seq"),
        P("rep", None, "seq"),
        P("rep", "seq", None),
        P(("groups", "seq"), None),
    )
    out_specs = (
        P(("groups", "seq"), "rep"),
        P(("groups", "seq"), "rep"),
        P(("groups", "seq"), None),
        P(("groups", "seq"), None),
    )
    return jax.shard_map(body, mesh=mesh, in_specs=in_specs, out_specs=out_specs, check_vma=False)
```
